32 devices in a mesh: cols: 4 (over y, x), dom: 8 (over z, core).
Axes of the slice: x: 2, y: 2, z: 4, core: 2. Of those that a mesh axis runs over, the one named last changes fastest.
Arguments:
- features: bfloat16 [768, 4096], P('cols', 'dom'), may hold values from -6 to 6
- proj_in: bfloat16 [768, 256], P('cols'), may hold values from -0.3125 to 0.3125
- self_weight: bfloat16 [256, 256], replicated, may hold values from -0.375 to 0.375
- neigh_weight: bfloat16 [256, 256], replicated, may hold values from -0.375 to 0.375
- neighbors: int32 [16, 4096], P(None, 'dom'), may hold values from 0 to 1023, as said below
- degree: int32 [4096], P('dom'), may hold values from 1 to 16
- send_rows: int32 [8, 512], P('dom'), may hold values from 0 to 511
- send_count: int32 [8, 8], P('dom'), may hold values from 0 to 64, as said below
Outputs:
- layer_out: bfloat16 [256, 4096], P('cols', 'dom')
The draws below stay inside these ranges and needn't reach their ends.
Inputs may be any that keep to these rules, and one draw needn't show every extreme that they name: `neighbors`: A code at or above 512 names a source partition other than the node's own and a slot below send_count of that source towards the node's partition. Every partition's rows are received in full (64 slots) from every other partition for at least one partition in every draw. `send_count`: zero on the diagonal; elsewhere 1 to 64, and 64 from every source towards at least one partition.
All inputs are finite; a program needn't handle non-finite values.
Results may differ from the reference program's by a relative error of at most 0.0051.
Values may be sent and summed in bfloat16 or wider, within the bound.
A program may use at most 64 MiB of HBM per device.

```python
import jax
import jax.numpy as jnp
from jax import lax

D_IN = 768
HID = 256
NODE_DEV = 512
K = 16
CAP = 64
NODES = 4096
N_DOM = 8


def shared_counts(key):
    base = jax.random.fold_in(key, 7)
    key_hot, key_pick, key_low = jax.random.split(base, 3)
    hot = jax.random.randint(key_hot, (N_DOM,), 0, 4) == 0
    chosen = jax.random.randint(key_pick, (), 0, N_DOM)
    hot = jnp.logical_or(hot, jnp.arange(N_DOM) == chosen)
    low = jax.random.randint(key_low, (N_DOM, N_DOM), 1, CAP // 2 + 1)
    counts = jnp.where(hot[None, :], CAP, low)
    diagonal = jnp.arange(N_DOM)[:, None] == jnp.arange(N_DOM)[None, :]
    counts = jnp.where(diagonal, 0, counts).astype(jnp.int32)
    return (counts, hot)


def draw_send_count(key, part):
    return shared_counts(key)[0]


def draw_neighbors(key, part):
    counts, hot = shared_counts(key)
    inner = jax.random.fold_in(key, 11)
    key_local, key_roll, key_source, key_slot = jax.random.split(inner, 4)
    part_of = (jnp.arange(NODES) // NODE_DEV)[:, None]
    local = jax.random.randint(key_local, (NODES, K), 0, NODE_DEV)
    roll = jax.random.randint(key_roll, (NODES, K), 0, 8)
    remote = roll < jnp.where(hot[part_of], 4, 1)
    source = (part_of + 1 + jax.random.randint(key_source, (NODES, K), 0, N_DOM - 1)) % N_DOM
    limit = counts[source, part_of]
    slot = jax.random.randint(key_slot, (NODES, K), 0, 1 << 20) % limit
    code = jnp.where(remote, NODE_DEV + source * CAP + slot, local)
    return code.T.astype(jnp.int32)


def with_ends(result, rng, smallest, top_value):
    extent = result.shape
    place = [jax.random.randint(jax.random.fold_in(rng, axis), (), 0, extent[axis]) for axis in range(len(extent))]
    result = result.at[tuple(place)].set(smallest)
    longest = extent.index(max(extent))
    place[longest] = (place[longest] + 1) % extent[longest]
    return result.at[tuple(place)].set(top_value)


def strengthened(entries, stream_key, source, target, shards_of, factor):
    owner, partner = [(jnp.arange(entries.shape[axis_at]) // (entries.shape[axis_at] // shards_of)).reshape([-1 if axis == axis_at else 1 for axis in range(entries.ndim)]) for axis_at in (source, target)]
    chosen = jax.random.permutation(stream_key, shards_of)[partner]
    strong = (owner == chosen) | (owner == (partner + shards_of // 2) % shards_of)
    return jnp.where(strong, factor * entries, entries)


def level_of(stream_key, shape, shards, least, high):
    gain = 1.0
    for axis_at, blocks in shards:
        heights = jax.random.uniform(jax.random.fold_in(jax.random.fold_in(stream_key, 6), axis_at), (blocks,), jnp.float32, least / len(shards), high / len(shards))
        gain = gain * jnp.repeat(jnp.exp(heights), shape[axis_at] // blocks).reshape((-1,) + (1,) * (len(shape) - 1 - axis_at))
    return gain


def noise(own_key, dims, deviation, most, cuts=(), kind=jnp.bfloat16):
    drawn = deviation * jax.random.normal(own_key, dims, jnp.float32)
    if cuts:
        drawn = drawn * level_of(own_key, dims, cuts, -0.22, 0.18)
    return jnp.clip(drawn, -most, most).astype(kind)


def bell_draw_with(stream_key, dims, width, reach, cuts, heavy, held_as=jnp.bfloat16):
    array = width * jax.random.normal(stream_key, dims, jnp.float32)
    if cuts:
        array = array * level_of(stream_key, dims, cuts, -0.22, 0.18)
    return jnp.clip(strengthened(array, jax.random.fold_in(stream_key, 3), *heavy), -reach, reach).astype(held_as)


def setup_inputs(seed: int = 0) -> dict:
    streams_of = jax.random.split(jax.random.key(seed), 9)
    features = noise(streams_of[0], (D_IN, NODES), 1.0, 6.0, ((0, 4), (1, 8)))
    proj_in = bell_draw_with(streams_of[1], (D_IN, HID), D_IN ** -0.5, 0.3125, ((0, 4),), (0, 1, 4, 2.0))
    self_weight = noise(streams_of[2], (HID, HID), HID ** -0.5, 0.375)
    neigh_weight = noise(streams_of[3], (HID, HID), HID ** -0.5, 0.375)
    neighbors = draw_neighbors(jax.random.fold_in(streams_of[8], 71), 0)
    degree = with_ends(jax.random.randint(streams_of[5], (NODES,), 1, K + 1), jax.random.fold_in(streams_of[5], 1), 1, K).astype(jnp.int32)
    send_rows = with_ends(jax.random.randint(streams_of[6], (N_DOM, N_DOM * CAP), 0, NODE_DEV), jax.random.fold_in(streams_of[6], 1), 0, NODE_DEV - 1).astype(jnp.int32)
    send_count = draw_send_count(jax.random.fold_in(streams_of[8], 71), 0)
    return dict(features=features, proj_in=proj_in, self_weight=self_weight, neigh_weight=neigh_weight, neighbors=neighbors, degree=degree, send_rows=send_rows, send_count=send_count)


def reference(features, proj_in, self_weight, neigh_weight, neighbors, degree, send_rows, send_count):
    hidden = jnp.dot(features.T, proj_in, preferred_element_type=jnp.float32).astype(jnp.bfloat16)
    codes = neighbors.T.reshape(N_DOM, NODE_DEV, K)
    degs = degree.reshape(N_DOM, NODE_DEV)
    parts = jnp.arange(N_DOM, dtype=jnp.int32)

    def one_part(inputs):
        code, deg, part = inputs
        remote = code >= NODE_DEV
        rel = jnp.maximum(code - NODE_DEV, 0)
        source = rel // CAP
        slot = rel % CAP
        sent = send_rows[source, part * CAP + slot]
        valid = slot < send_count[source, part]
        rows = jnp.where(remote, source * NODE_DEV + sent, part * NODE_DEV + code).astype(jnp.int32)
        used = jnp.arange(K, dtype=jnp.int32)[None, :] < deg[:, None]
        keep = jnp.logical_and(used, jnp.logical_or(jnp.logical_not(remote), valid))
        picked = hidden[rows].astype(jnp.float32)
        total = jnp.sum(jnp.where(keep[:, :, None], picked, jnp.float32(0.0)), axis=1)
        return (total / deg[:, None].astype(jnp.float32)).astype(jnp.bfloat16)

    mean = lax.map(one_part, (codes, degs, parts)).reshape(NODES, HID)
    total = jnp.dot(hidden, self_weight, preferred_element_type=jnp.float32)
    total = total + jnp.dot(mean, neigh_weight, preferred_element_type=jnp.float32)
    return jnp.maximum(total, 0.0).astype(jnp.bfloat16).T
```

```python
import functools
import math

import jax
import jax.numpy as jnp
from jax import lax
from jax.experimental import pallas as pl
from jax.experimental.pallas import tpu as pltpu
from jax.sharding import PartitionSpec as P

MESH = pl.DeviceIdType.MESH
LANES = 128


def dot(left, right, left_dim, right_dim):
    return lax.dot_general(
        left, right, (((left_dim,), (right_dim,)), ((), ())), preferred_element_type=jnp.float32
    )


def kernel(
    cols,
    parts,
    capacity,
    feat_hbm,
    proj_hbm,
    selfw_hbm,
    neighw_hbm,
    neigh_hbm,
    degree_hbm,
    rows_hbm,
    count_hbm,
    out_ref,
    feat,
    proj,
    selfw,
    neighw,
    neigh,
    degree,
    rows,
    count,
    own,
    own_self,
    outgoing_sum,
    outgoing_self,
    incoming_sum,
    incoming_self,
    reduced,
    pick,
    packed_out,
    packed_in,
    table,
    counts,
    in_sem,
    sum_send,
    sum_recv,
    row_send,
    row_recv,
    self_send,
    self_recv,
):
    column = lax.axis_index("cols")
    part = lax.axis_index("dom")
    width = out_ref.shape[0]
    nodes = out_ref.shape[1]
    hid = width * cols
    slots = rows.shape[1]
    slot_count = neigh.shape[0]
    fold = LANES // capacity
    short = width // fold

    loads = [
        pltpu.make_async_copy(source, target, in_sem.at[i])
        for i, (source, target) in enumerate(
            (
                (feat_hbm, feat),
                (proj_hbm, proj),
                (neighw_hbm, neighw),
                (selfw_hbm, selfw),
                (rows_hbm, rows),
                (count_hbm, count),
                (neigh_hbm, neigh),
                (degree_hbm, degree),
            )
        )
    ]
    for load in loads:
        load.start()

    barrier = pltpu.get_barrier_semaphore()
    for step in range(1, cols):
        pl.semaphore_signal(
            barrier, inc=1, device_id=((column + step) % cols, part), device_id_type=MESH
        )

    def greet(step, carry):
        pl.semaphore_signal(
            barrier, inc=1, device_id=(column, (part + step) % parts), device_id_type=MESH
        )
        return carry

    lax.fori_loop(1, parts, greet, 0)

    for load in loads[:3]:
        load.wait()
    to_neigh = dot(proj[...], neighw[...], 1, 0).astype(jnp.bfloat16)
    value = dot(to_neigh, feat[...], 0, 0)
    own[...] = value
    outgoing_sum[...] = value.astype(outgoing_sum.dtype)
    pl.semaphore_wait(barrier, cols + parts - 2)

    def band(index):
        return pl.ds(pl.multiple_of(index * width, width), width)

    def other(step, me, count):
        return step - 1 + (step - 1 + count - me) // count

    def scatter(outgoing, incoming, send, recv):
        copies = []
        for step in range(1, cols):
            peer = other(step, column, cols)
            copies.append(
                pltpu.make_async_remote_copy(
                    src_ref=outgoing.at[band(peer)],
                    dst_ref=incoming.at[column],
                    send_sem=send.at[step - 1],
                    recv_sem=recv.at[column],
                    device_id=(peer, part),
                    device_id_type=MESH,
                )
            )
        return copies

    def arrivals(outgoing, incoming, send, recv):
        copies = []
        for step in range(1, cols):
            peer = other(step, column, cols)
            copies.append(
                pltpu.make_async_remote_copy(
                    src_ref=outgoing.at[band(peer)],
                    dst_ref=incoming.at[peer],
                    send_sem=send.at[step - 1],
                    recv_sem=recv.at[peer],
                    device_id=(peer, part),
                    device_id_type=MESH,
                )
            )
        return copies

    sums = scatter(outgoing_sum, incoming_sum, sum_send, sum_recv)
    for copy in sums:
        copy.start()

    loads[3].wait()
    to_self = dot(proj[...], selfw[...], 1, 0).astype(jnp.bfloat16)
    value = dot(to_self, feat[...], 0, 0)
    own_self[...] = value
    outgoing_self[...] = value.astype(outgoing_self.dtype)
    selves = scatter(outgoing_self, incoming_self, self_send, self_recv)
    for copy in selves:
        copy.start()

    for load in loads[4:]:
        load.wait()
    group = min(slots, 512)
    spread = group * fold

    def choose(index, carry):
        start = pl.multiple_of(index * group, group)
        wanted = rows[:, pl.ds(start, group)]
        source = (
            lax.broadcasted_iota(jnp.int32, (parts, group), 1) + start
        ) // capacity == lax.broadcasted_iota(jnp.int32, (parts, group), 0)
        amount = dot(
            jnp.broadcast_to(count[...].astype(jnp.float32), (8, parts)).astype(jnp.bfloat16),
            source.astype(jnp.float32).astype(jnp.bfloat16),
            1,
            0,
        )[0:1, :]
        slot = (lax.broadcasted_iota(jnp.int32, (1, group), 1) % capacity).astype(jnp.float32)
        wanted = jnp.where(slot < amount, wanted, -1)
        pieces = []
        for block in range(group // capacity):
            piece = wanted[:, block * capacity : (block + 1) * capacity]
            pieces += [piece] * fold
        wide = jnp.concatenate(pieces, axis=1)
        hit = lax.broadcasted_iota(jnp.int32, (nodes, spread), 0) == wide
        pick[:, pl.ds(pl.multiple_of(index * spread, spread), spread)] = jnp.where(
            hit, 1.0, 0.0
        ).astype(jnp.bfloat16)
        return carry

    lax.fori_loop(0, slots // group, choose, 0)

    used = lax.broadcasted_iota(jnp.int32, (slot_count, nodes), 0) < degree[...]
    codes = jnp.where(used, neigh[...], -1)
    neigh[...] = codes
    depth = 256
    row_of = lax.broadcasted_iota(jnp.int32, (depth, LANES), 0).astype(jnp.float32).astype(jnp.bfloat16)
    one = jnp.ones((depth, LANES), jnp.bfloat16)
    zero = jnp.zeros((depth, LANES), jnp.bfloat16)

    def tally(index, carry):
        start = pl.multiple_of(index * depth, depth)
        for lane in range(nodes // LANES):
            there = slice(lane * LANES, (lane + 1) * LANES)
            near = jnp.clip(neigh[:, there] - start, -1, depth).astype(jnp.float32)
            total = zero
            for slot in range(slot_count):
                code = jnp.broadcast_to(near[slot : slot + 1, :], (16, LANES)).astype(jnp.bfloat16)
                code = jnp.concatenate([code] * (depth // 16), axis=0)
                total = total + jnp.where(row_of == code, one, zero)
            counts[pl.ds(start, depth), there] = total
        return carry

    lax.fori_loop(0, counts.shape[0] // depth, tally, 0)

    def total_of(mine, copies, incoming):
        for copy in copies:
            copy.wait_recv()
        total = mine[band(column), :]
        for step in range(1, cols):
            total = total + incoming[other(step, column, cols)].astype(jnp.float32)
        return total

    total = total_of(own, arrivals(outgoing_sum, incoming_sum, sum_send, sum_recv), incoming_sum)
    reduced[...] = total.astype(jnp.bfloat16)

    folded = lax.broadcasted_iota(jnp.int32, (short, spread), 1) % LANES // capacity

    def pack(index, carry):
        start = pl.multiple_of(index * spread, spread)
        chosen = dot(reduced[...], pick[:, pl.ds(start, spread)], 1, 0)
        tight = chosen[0:short, :]
        for piece in range(1, fold):
            tight = jnp.where(folded == piece, chosen[piece * short : (piece + 1) * short, :], tight)
        tight = tight.astype(jnp.bfloat16)
        for block in range(spread // LANES):
            packed_out[index * (spread // LANES) + block] = tight[:, block * LANES : (block + 1) * LANES]
        return carry

    lax.fori_loop(0, slots // group, pack, 0)

    def to_part(step):
        peer = other(step, part, parts)
        return pltpu.make_async_remote_copy(
            src_ref=packed_out.at[peer],
            dst_ref=packed_in.at[part],
            send_sem=row_send.at[step],
            recv_sem=row_recv.at[part],
            device_id=(column, peer),
            device_id_type=MESH,
        )

    def from_part(step):
        peer = other(step, part, parts)
        return pltpu.make_async_remote_copy(
            src_ref=packed_out.at[peer],
            dst_ref=packed_in.at[peer],
            send_sem=row_send.at[step],
            recv_sem=row_recv.at[peer],
            device_id=(column, peer),
            device_id_type=MESH,
        )

    def send_rows(step, carry):
        to_part(step).start()
        return carry

    lax.fori_loop(1, parts, send_rows, 0)

    packed_in[part] = jnp.zeros((short, LANES), jnp.bfloat16)
    local_sum = dot(reduced[...], counts[0:nodes, :], 1, 0)

    def arrive(step, carry):
        from_part(step).wait_recv()
        return carry

    lax.fori_loop(1, parts, arrive, 0)

    half = lax.broadcasted_iota(jnp.int32, (short, LANES), 1) // capacity

    def unpack(index, carry):
        for piece in range(fold):
            value = jnp.zeros((short, LANES), jnp.float32)
            for place in range(fold):
                block = packed_in[index * fold + place].astype(jnp.float32)
                shift = (place - piece) * capacity % LANES
                if shift:
                    block = pltpu.roll(block, shift, 1)
                value = jnp.where(half == place, block, value)
            table[piece * short : (piece + 1) * short, pl.ds(pl.multiple_of(index * LANES, LANES), LANES)] = (
                value.astype(jnp.bfloat16)
            )
        return carry

    lax.fori_loop(0, parts // fold, unpack, 0)
    summed = local_sum + dot(table[...], counts[nodes:, :], 1, 0)
    result = summed / degree[...].astype(jnp.float32)
    result = result + total_of(
        own_self, arrivals(outgoing_self, incoming_self, self_send, self_recv), incoming_self
    )
    out_ref[...] = jnp.maximum(result, 0.0).astype(out_ref.dtype)

    for copy in sums + selves:
        copy.wait_send()

    def sent(step, carry):
        to_part(step).wait_send()
        return carry

    lax.fori_loop(1, parts, sent, 0)


def local(features, proj_in, self_weight, neigh_weight, neighbors, degree, send_rows, send_count):
    cols = lax.axis_size("cols")
    parts = lax.axis_size("dom")
    hid = proj_in.shape[1]
    width = hid // cols
    nodes = features.shape[1]
    slots = send_rows.shape[1]
    capacity = slots // parts
    fold = LANES // capacity
    short = width // fold
    degree = degree.reshape(1, nodes)
    arguments = (
        features,
        proj_in,
        self_weight,
        neigh_weight,
        neighbors,
        degree,
        send_rows,
        send_count,
    )
    bf16 = jnp.bfloat16
    copies = pltpu.SemaphoreType.DMA
    return pl.pallas_call(
        functools.partial(kernel, cols, parts, capacity),
        out_shape=jax.ShapeDtypeStruct((width, nodes), bf16),
        in_specs=[pl.BlockSpec(memory_space=pltpu.HBM)] * len(arguments),
        out_specs=pl.BlockSpec(memory_space=pltpu.VMEM),
        scratch_shapes=[pltpu.VMEM(a.shape, a.dtype) for a in arguments]
        + [
            pltpu.VMEM((hid, nodes), jnp.float32),
            pltpu.VMEM((hid, nodes), jnp.float32),
            pltpu.VMEM((hid, nodes), bf16),
            pltpu.VMEM((hid, nodes), bf16),
            pltpu.VMEM((cols, width, nodes), bf16),
            pltpu.VMEM((cols, width, nodes), bf16),
            pltpu.VMEM((width, nodes), bf16),
            pltpu.VMEM((nodes, slots * fold), bf16),
            pltpu.VMEM((parts, short, LANES), bf16),
            pltpu.VMEM((parts, short, LANES), bf16),
            pltpu.VMEM((width, slots), bf16),
            pltpu.VMEM((nodes + slots, nodes), bf16),
            copies((len(arguments),)),
            copies((cols - 1,)),
            copies((cols,)),
            copies((parts,)),
            copies((parts,)),
            copies((cols - 1,)),
            copies((cols,)),
        ],
        compiler_params=pltpu.CompilerParams(
            collective_id=0, has_side_effects=True, vmem_limit_bytes=67043328
        ),
        name="layer",
    )(*arguments)


def solution(mesh):
    return jax.shard_map(
        local,
        mesh=mesh,
        in_specs=(
            P("cols", "dom"),
            P("cols", None),
            P(),
            P(),
            P(None, "dom"),
            P("dom"),
            P("dom", None),
            P("dom", None),
        ),
        out_specs=P("cols", "dom"),
        check_vma=False,
    )
```

```python
import functools
import math

import jax
import jax.numpy as jnp
from jax import lax
from jax.experimental import pallas as pl
from jax.experimental.pallas import tpu as pltpu
from jax.sharding import PartitionSpec as P

MESH = pl.DeviceIdType.MESH
LANES = 128


def dot(left, right, left_dim, right_dim):
    return lax.dot_general(
        left, right, (((left_dim,), (right_dim,)), ((), ())), preferred_element_type=jnp.float32
    )


def kernel(
    cols,
    parts,
    capacity,
    feat_hbm,
    proj_hbm,
    selfw_hbm,
    neighw_hbm,
    neigh_hbm,
    degree_hbm,
    rows_hbm,
    count_hbm,
    out_ref,
    feat,
    proj,
    selfw,
    neighw,
    neigh,
    degree,
    rows,
    count,
    own,
    own_self,
    outgoing_sum,
    outgoing_self,
    incoming_sum,
    incoming_self,
    reduced,
    pick,
    packed_out,
    packed_in,
    table,
    counts,
    in_sem,
    sum_send,
    sum_recv,
    row_send,
    row_recv,
    self_send,
    self_recv,
):
    column = lax.axis_index("cols")
    part = lax.axis_index("dom")
    width = out_ref.shape[0]
    nodes = out_ref.shape[1]
    hid = width * cols
    slots = rows.shape[1]
    slot_count = neigh.shape[0]
    fold = LANES // capacity
    short = width // fold

    loads = [
        pltpu.make_async_copy(source, target, in_sem.at[i])
        for i, (source, target) in enumerate(
            (
                (feat_hbm, feat),
                (proj_hbm, proj),
                (neighw_hbm, neighw),
                (selfw_hbm, selfw),
                (rows_hbm, rows),
                (count_hbm, count),
                (neigh_hbm, neigh),
                (degree_hbm, degree),
            )
        )
    ]
    for load in loads:
        load.start()

    barrier = pltpu.get_barrier_semaphore()
    for step in range(1, cols):
        pl.semaphore_signal(
            barrier, inc=1, device_id=((column + step) % cols, part), device_id_type=MESH
        )

    def greet(step, carry):
        pl.semaphore_signal(
            barrier, inc=1, device_id=(column, (part + step) % parts), device_id_type=MESH
        )
        return carry

    lax.fori_loop(1, parts, greet, 0)

    for load in loads[:3]:
        load.wait()
    to_neigh = dot(proj[...], neighw[...], 1, 0).astype(jnp.bfloat16)
    value = dot(to_neigh, feat[...], 0, 0)
    own[...] = value
    outgoing_sum[...] = value.astype(outgoing_sum.dtype)
    pl.semaphore_wait(barrier, cols + parts - 2)

    def band(index):
        return pl.ds(pl.multiple_of(index * width, width), width)

    def other(step, me, count):
        return step - 1 + (step - 1 + count - me) // count

    def scatter(outgoing, incoming, send, recv):
        copies = []
        for step in range(1, cols):
            peer = other(step, column, cols)
            copies.append(
                pltpu.make_async_remote_copy(
                    src_ref=outgoing.at[band(peer)],
                    dst_ref=incoming.at[column],
                    send_sem=send.at[step - 1],
                    recv_sem=recv.at[column],
                    device_id=(peer, part),
                    device_id_type=MESH,
                )
            )
        return copies

    def arrivals(outgoing, incoming, send, recv):
        copies = []
        for step in range(1, cols):
            peer = other(step, column, cols)
            copies.append(
                pltpu.make_async_remote_copy(
                    src_ref=outgoing.at[band(peer)],
                    dst_ref=incoming.at[peer],
                    send_sem=send.at[step - 1],
                    recv_sem=recv.at[peer],
                    device_id=(peer, part),
                    device_id_type=MESH,
                )
            )
        return copies

    sums = scatter(outgoing_sum, incoming_sum, sum_send, sum_recv)
    for copy in sums:
        copy.start()

    loads[3].wait()
    to_self = dot(proj[...], selfw[...], 1, 0).astype(jnp.bfloat16)
    value = dot(to_self, feat[...], 0, 0)
    own_self[...] = value
    outgoing_self[...] = value.astype(outgoing_self.dtype)
    selves = scatter(outgoing_self, incoming_self, self_send, self_recv)
    for copy in selves:
        copy.start()

    for load in loads[4:]:
        load.wait()
    group = min(slots, 512)
    spread = group * fold

    def choose(index, carry):
        start = pl.multiple_of(index * group, group)
        wanted = rows[:, pl.ds(start, group)]
        source = (
            lax.broadcasted_iota(jnp.int32, (parts, group), 1) + start
        ) // capacity == lax.broadcasted_iota(jnp.int32, (parts, group), 0)
        amount = dot(
            jnp.broadcast_to(count[...].astype(jnp.float32), (8, parts)).astype(jnp.bfloat16),
            source.astype(jnp.float32).astype(jnp.bfloat16),
            1,
            0,
        )[0:1, :]
        slot = (lax.broadcasted_iota(jnp.int32, (1, group), 1) % capacity).astype(jnp.float32)
        wanted = jnp.where(slot < amount, wanted, -1)
        pieces = []
        for block in range(group // capacity):
            piece = wanted[:, block * capacity : (block + 1) * capacity]
            pieces += [piece] * fold
        wide = jnp.concatenate(pieces, axis=1)
        hit = lax.broadcasted_iota(jnp.int32, (nodes, spread), 0) == wide
        pick[:, pl.ds(pl.multiple_of(index * spread, spread), spread)] = jnp.where(
            hit, 1.0, 0.0
        ).astype(jnp.bfloat16)
        return carry

    lax.fori_loop(0, slots // group, choose, 0)

    used = lax.broadcasted_iota(jnp.int32, (slot_count, nodes), 0) < degree[...]
    codes = jnp.where(used, neigh[...], -1)
    neigh[...] = codes
    depth = 256
    row_of = lax.broadcasted_iota(jnp.int32, (depth, LANES), 0).astype(jnp.float32).astype(jnp.bfloat16)
    one = jnp.ones((depth, LANES), jnp.bfloat16)
    zero = jnp.zeros((depth, LANES), jnp.bfloat16)

    def tally(index, carry):
        start = pl.multiple_of(index * depth, depth)
        for lane in range(nodes // LANES):
            there = slice(lane * LANES, (lane + 1) * LANES)
            near = jnp.clip(neigh[:, there] - start, -1, depth).astype(jnp.float32)
            total = zero
            for slot in range(slot_count):
                code = jnp.broadcast_to(near[slot : slot + 1, :], (16, LANES)).astype(jnp.bfloat16)
                code = jnp.concatenate([code] * (depth // 16), axis=0)
                total = total + jnp.where(row_of == code, one, zero)
            counts[pl.ds(start, depth), there] = total
        return carry

    lax.fori_loop(0, counts.shape[0] // depth, tally, 0)

    def total_of(mine, copies, incoming):
        for copy in copies:
            copy.wait_recv()
        total = mine[band(column), :]
        for step in range(1, cols):
            total = total + incoming[other(step, column, cols)].astype(jnp.float32)
        return total

    total = total_of(own, arrivals(outgoing_sum, incoming_sum, sum_send, sum_recv), incoming_sum)
    reduced[...] = total.astype(jnp.bfloat16)

    folded = lax.broadcasted_iota(jnp.int32, (short, spread), 1) % LANES // capacity

    def pack(index, carry):
        start = pl.multiple_of(index * spread, spread)
        chosen = dot(reduced[...], pick[:, pl.ds(start, spread)], 1, 0)
        tight = chosen[0:short, :]
        for piece in range(1, fold):
            tight = jnp.where(folded == piece, chosen[piece * short : (piece + 1) * short, :], tight)
        tight = tight.astype(jnp.bfloat16)
        for block in range(spread // LANES):
            packed_out[index * (spread // LANES) + block] = tight[:, block * LANES : (block + 1) * LANES]
        return carry

    lax.fori_loop(0, slots // group, pack, 0)

    def to_part(step):
        peer = other(step, part, parts)
        return pltpu.make_async_remote_copy(
            src_ref=packed_out.at[peer],
            dst_ref=packed_in.at[part],
            send_sem=row_send.at[step],
            recv_sem=row_recv.at[part],
            device_id=(column, peer),
            device_id_type=MESH,
        )

    def from_part(step):
        peer = other(step, part, parts)
        return pltpu.make_async_remote_copy(
            src_ref=packed_out.at[peer],
            dst_ref=packed_in.at[peer],
            send_sem=row_send.at[step],
            recv_sem=row_recv.at[peer],
            device_id=(column, peer),
            device_id_type=MESH,
        )

    def send_rows(step, carry):
        to_part(step).start()
        return carry

    lax.fori_loop(1, parts, send_rows, 0)

    packed_in[part] = jnp.zeros((short, LANES), jnp.bfloat16)
    local_sum = dot(reduced[...], counts[0:nodes, :], 1, 0)

    def arrive(step, carry):
        from_part(step).wait_recv()
        return carry

    lax.fori_loop(1, parts, arrive, 0)

    half = lax.broadcasted_iota(jnp.int32, (short, LANES), 1) // capacity

    def unpack(index, carry):
        for piece in range(fold):
            value = jnp.zeros((short, LANES), jnp.float32)
            for place in range(fold):
                block = packed_in[index * fold + place].astype(jnp.float32)
                shift = (place - piece) * capacity % LANES
                if shift:
                    block = pltpu.roll(block, shift, 1)
                value = jnp.where(half == place, block, value)
            table[piece * short : (piece + 1) * short, pl.ds(pl.multiple_of(index * LANES, LANES), LANES)] = (
                value.astype(jnp.bfloat16)
            )
        return carry

    lax.fori_loop(0, parts // fold, unpack, 0)
    summed = local_sum + dot(table[...], counts[nodes:, :], 1, 0)
    result = summed / degree[...].astype(jnp.float32)
    result = result + total_of(
        own_self, arrivals(outgoing_self, incoming_self, self_send, self_recv), incoming_self
    )
    out_ref[...] = jnp.maximum(result, 0.0).astype(out_ref.dtype)

    for copy in sums + selves:
        copy.wait_send()

    def sent(step, carry):
        to_part(step).wait_send()
        return carry

    lax.fori_loop(1, parts, sent, 0)


def local(features, proj_in, self_weight, neigh_weight, neighbors, degree, send_rows, send_count):
    cols = lax.axis_size("cols")
    parts = lax.axis_size("dom")
    hid = proj_in.shape[1]
    width = hid // cols
    nodes = features.shape[1]
    slots = send_rows.shape[1]
    capacity = slots // parts
    fold = LANES // capacity
    short = width // fold
    degree = degree.reshape(1, nodes)
    arguments = (
        features,
        proj_in,
        self_weight,
        neigh_weight,
        neighbors,
        degree,
        send_rows,
        send_count,
    )
    bf16 = jnp.bfloat16
    copies = pltpu.SemaphoreType.DMA
    limit = (16 << 20) + (slots * nodes * (fold + 1) + hid * nodes * 16) * 2
    return pl.pallas_call(
        functools.partial(kernel, cols, parts, capacity),
        out_shape=jax.ShapeDtypeStruct((width, nodes), bf16),
        in_specs=[pl.BlockSpec(memory_space=pltpu.HBM)] * len(arguments),
        out_specs=pl.BlockSpec(memory_space=pltpu.VMEM),
        scratch_shapes=[pltpu.VMEM(a.shape, a.dtype) for a in arguments]
        + [
            pltpu.VMEM((hid, nodes), jnp.float32),
            pltpu.VMEM((hid, nodes), jnp.float32),
            pltpu.VMEM((hid, nodes), bf16),
            pltpu.VMEM((hid, nodes), bf16),
            pltpu.VMEM((cols, width, nodes), bf16),
            pltpu.VMEM((cols, width, nodes), bf16),
            pltpu.VMEM((width, nodes), bf16),
            pltpu.VMEM((nodes, slots * fold), bf16),
            pltpu.VMEM((parts, short, LANES), bf16),
            pltpu.VMEM((parts, short, LANES), bf16),
            pltpu.VMEM((width, slots), bf16),
            pltpu.VMEM((nodes + slots, nodes), bf16),
            copies((len(arguments),)),
            copies((cols - 1,)),
            copies((cols,)),
            copies((parts,)),
            copies((parts,)),
            copies((cols - 1,)),
            copies((cols,)),
        ],
        compiler_params=pltpu.CompilerParams(
            collective_id=0, has_side_effects=True, vmem_limit_bytes=limit
        ),
        name="layer",
    )(*[pltpu.with_memory_space_constraint(a, pltpu.HBM) for a in arguments])


def solution(mesh):
    return jax.shard_map(
        local,
        mesh=mesh,
        in_specs=(
            P("cols", "dom"),
            P("cols", None),
            P(),
            P(),
            P(None, "dom"),
            P("dom"),
            P("dom", None),
            P("dom", None),
        ),
        out_specs=P("cols", "dom"),
        check_vma=False,
    )
```

```python
import functools

import jax
import jax.numpy as jnp
from jax import lax
from jax.experimental import pallas as pl
from jax.experimental.pallas import tpu as pltpu
from jax.sharding import PartitionSpec as P

MESH = pl.DeviceIdType.MESH
LANES = 128
CHUNKS = 4


def dot(left, right, left_dim, right_dim):
    return lax.dot_general(
        left, right, (((left_dim,), (right_dim,)), ((), ())), preferred_element_type=jnp.float32
    )


def partner(me, step, count):
    if count & (count - 1):
        return (me + step) % count
    other = me
    for bit in range(count.bit_length()):
        if step >> bit & 1:
            size = 1 << bit
            other = other + size - 2 * size * (me // size % 2)
    return other


def kernel(
    cols,
    parts,
    capacity,
    feat_hbm,
    proj_hbm,
    selfw_hbm,
    neighw_hbm,
    neigh_hbm,
    degree_hbm,
    rows_hbm,
    count_hbm,
    out_ref,
    feat,
    proj,
    selfw,
    neighw,
    neigh,
    degree,
    rows,
    count,
    weights,
    weights_self,
    projected,
    own,
    own_self,
    outgoing_sum,
    outgoing_self,
    incoming_sum,
    incoming_self,
    pick,
    packed_out,
    packed_in,
    remote,
    counts,
    in_sem,
    sum_send,
    sum_recv,
    row_send,
    row_recv,
    self_send,
    self_recv,
):
    column = lax.axis_index("cols")
    part = lax.axis_index("dom")
    width = out_ref.shape[0]
    nodes = out_ref.shape[1]
    slots = rows.shape[1]
    slot_count = neigh.shape[0]
    fold = LANES // capacity
    short = width // fold
    pairs = parts // fold
    steps = sorted(range(1, cols), key=lambda step: -bin(step).count("1"))

    loads = [
        pltpu.make_async_copy(source, target, in_sem.at[i])
        for i, (source, target) in enumerate(
            (
                (rows_hbm, rows),
                (count_hbm, count),
                (neighw_hbm, neighw),
                (proj_hbm, proj),
                (feat_hbm, feat),
                (selfw_hbm, selfw),
                (neigh_hbm, neigh),
                (degree_hbm, degree),
            )
        )
    ]
    for load in loads:
        load.start()

    barrier = pltpu.get_barrier_semaphore()
    for step in range(1, cols):
        pl.semaphore_signal(
            barrier, inc=1, device_id=((column + step) % cols, part), device_id_type=MESH
        )

    def greet(step, carry):
        pl.semaphore_signal(
            barrier, inc=1, device_id=(column, (part + step) % parts), device_id_type=MESH
        )
        return carry

    lax.fori_loop(1, parts, greet, 0)

    def band(index):
        return pl.ds(pl.multiple_of(index * width, width), width)

    def scatter(source, target, send, recv, peer):
        return pltpu.make_async_remote_copy(
            src_ref=source,
            dst_ref=target,
            send_sem=send,
            recv_sem=recv,
            device_id=(peer, part),
            device_id_type=MESH,
        )

    def sum_copy(chunk, step, arriving=False):
        peer = partner(column, step, cols)
        slot = peer if arriving else column
        return scatter(
            outgoing_sum.at[chunk, band(peer)],
            incoming_sum.at[chunk, slot],
            sum_send.at[chunk, step - 1],
            sum_recv.at[chunk, slot],
            peer,
        )

    def self_copy(step, arriving=False):
        peer = partner(column, step, cols)
        slot = peer if arriving else column
        return scatter(
            outgoing_self.at[band(peer)],
            incoming_self.at[slot],
            self_send.at[step - 1],
            self_recv.at[slot],
            peer,
        )

    group = min(slots, 512)

    def choose(index, carry):
        start = pl.multiple_of(index * group, group)
        wanted = rows[:, pl.ds(start, group)]
        source = (
            lax.broadcasted_iota(jnp.int32, (parts, group), 1) + start
        ) // capacity == lax.broadcasted_iota(jnp.int32, (parts, group), 0)
        amount = dot(
            jnp.broadcast_to(count[...].astype(jnp.float32), (8, parts)).astype(jnp.bfloat16),
            source.astype(jnp.float32).astype(jnp.bfloat16),
            1,
            0,
        )[0:1, :]
        slot = (lax.broadcasted_iota(jnp.int32, (1, group), 1) % capacity).astype(jnp.float32)
        wanted = jnp.where(slot < amount, wanted, -1)
        hit = lax.broadcasted_iota(jnp.int32, (nodes, group), 0) == wanted
        pick[:, pl.ds(start, group)] = jnp.where(hit, 1.0, 0.0).astype(jnp.bfloat16)
        return carry

    lanes = slots // CHUNKS
    rate = parts // CHUNKS
    for load in loads[2:4]:
        load.wait()
    weights[...] = dot(neighw[...], proj[...], 0, 1).astype(jnp.bfloat16)
    for load in loads[:2]:
        load.wait()
    lax.fori_loop(0, slots // group, choose, 0)
    loads[4].wait()
    projected[...] = dot(weights[...], feat[...], 1, 0).astype(jnp.bfloat16)
    pl.semaphore_wait(barrier, cols + parts - 2)
    for chunk in range(CHUNKS):
        outgoing_sum[chunk] = dot(
            projected[...], pick[:, chunk * lanes : (chunk + 1) * lanes], 1, 0
        ).astype(jnp.bfloat16)
        for step in steps:
            sum_copy(chunk, step).start()
    for chunk in range(CHUNKS):
        own[chunk] = outgoing_sum[chunk, band(column), :]
    for load in loads[5:]:
        load.wait()
    weights_self[...] = dot(selfw[...], proj[...], 0, 1).astype(jnp.bfloat16)
    used = lax.broadcasted_iota(jnp.int32, (slot_count, nodes), 0) < degree[...]
    codes = jnp.where(used, neigh[...], -1)
    neigh[...] = codes
    depth = 256
    row_of = lax.broadcasted_iota(jnp.int32, (depth, LANES), 0).astype(jnp.float32).astype(jnp.bfloat16)
    one = jnp.ones((depth, LANES), jnp.bfloat16)
    zero = jnp.zeros((depth, LANES), jnp.bfloat16)

    def tally(index, carry):
        start = pl.multiple_of(index * depth, depth)
        for lane in range(nodes // LANES):
            there = slice(lane * LANES, (lane + 1) * LANES)
            near = jnp.clip(neigh[:, there] - start, -1, depth).astype(jnp.float32)
            total = zero
            for slot in range(slot_count):
                code = jnp.broadcast_to(near[slot : slot + 1, :], (16, LANES)).astype(jnp.bfloat16)
                code = jnp.concatenate([code] * (depth // 16), axis=0)
                total = total + jnp.where(row_of == code, one, zero)
            counts[pl.ds(start, depth), there] = total
        return carry

    lax.fori_loop(0, nodes // depth, tally, 0)
    share = 1.0 / degree[...].astype(jnp.float32)
    value = dot(projected[...], counts[0:nodes, :], 1, 0) * share
    value = value + dot(weights_self[...], feat[...], 1, 0)
    outgoing_self[...] = value.astype(jnp.bfloat16)
    for step in steps:
        self_copy(step).start()
    own_self[...] = outgoing_self[band(column), :].astype(jnp.float32)
    lax.fori_loop(nodes // depth, counts.shape[0] // depth, tally, 0)
    packed_in[part] = jnp.zeros((short, LANES), jnp.bfloat16)

    def part_copy(peer, slot):
        return pltpu.make_async_remote_copy(
            src_ref=packed_out.at[peer],
            dst_ref=packed_in.at[slot],
            send_sem=row_send.at[peer],
            recv_sem=row_recv.at[slot],
            device_id=(column, peer),
            device_id_type=MESH,
        )

    half = lax.broadcasted_iota(jnp.int32, (short, LANES), 1) // capacity

    for chunk in range(CHUNKS):
        for step in steps:
            sum_copy(chunk, step, True).wait_recv()
        total = own[chunk].astype(jnp.float32)
        for step in steps:
            total = total + incoming_sum[chunk, partner(column, step, cols)].astype(jnp.float32)
        first = chunk * rate
        for place in range(rate):
            block = total[:, place // fold * LANES : (place // fold + 1) * LANES]
            tight = None
            for piece in range(fold):
                shift = (piece - place % fold) * capacity % LANES
                value = block[piece * short : (piece + 1) * short, :]
                value = pltpu.roll(value, shift, 1) if shift else value
                tight = value if tight is None else jnp.where(half == piece, value, tight)
            packed_out[first + place] = tight.astype(jnp.bfloat16)
        for place in range(rate):

            @pl.when(first + place != part)
            def _():
                part_copy(first + place, part).start()

    remote[...] = jnp.zeros((width, nodes), jnp.float32)

    def gather(turn, carry):
        pair = (part // fold + turn) % pairs
        blocks = []
        for place in range(fold):
            peer = pair * fold + place

            @pl.when(peer != part)
            def _():
                part_copy(peer, peer).wait_recv()

        for place in range(fold):
            blocks.append(packed_in[pair * fold + place].astype(jnp.float32))
        pieces = []
        for piece in range(fold):
            value = jnp.zeros((short, LANES), jnp.float32)
            for place in range(fold):
                shift = (place - piece) * capacity % LANES
                block = pltpu.roll(blocks[place], shift, 1) if shift else blocks[place]
                value = jnp.where(half == place, block, value)
            pieces.append(value)
        table = jnp.concatenate(pieces, axis=0).astype(jnp.bfloat16)
        start = pl.multiple_of(nodes + pair * LANES, LANES)
        remote[...] += dot(table, counts[pl.ds(start, LANES), :], 1, 0)
        return carry

    lax.fori_loop(0, pairs, gather, 0)
    total = own_self[...]
    for step in steps:
        self_copy(step, True).wait_recv()
    for step in steps:
        total = total + incoming_self[partner(column, step, cols)].astype(jnp.float32)
    result = total + remote[...] * share
    out_ref[...] = jnp.maximum(result, 0.0).astype(out_ref.dtype)
    for step in steps:
        for chunk in range(CHUNKS):
            sum_copy(chunk, step).wait_send()
        self_copy(step).wait_send()

    def sent(peer, carry):
        @pl.when(peer != part)
        def _():
            part_copy(peer, part).wait_send()

        return carry

    lax.fori_loop(0, parts, sent, 0)


def local(features, proj_in, self_weight, neigh_weight, neighbors, degree, send_rows, send_count):
    cols = lax.axis_size("cols")
    parts = lax.axis_size("dom")
    inputs, hid = proj_in.shape
    width = hid // cols
    nodes = features.shape[1]
    slots = send_rows.shape[1]
    capacity = slots // parts
    fold = LANES // capacity
    short = width // fold
    degree = degree.reshape(1, nodes)
    arguments = (
        features,
        proj_in,
        self_weight,
        neigh_weight,
        neighbors,
        degree,
        send_rows,
        send_count,
    )
    bf16 = jnp.bfloat16
    copies = pltpu.SemaphoreType.DMA
    limit = (16 << 20) + (slots * nodes + slots * hid + hid * nodes * 8) * 4
    return pl.pallas_call(
        functools.partial(kernel, cols, parts, capacity),
        out_shape=jax.ShapeDtypeStruct((width, nodes), bf16),
        in_specs=[pl.BlockSpec(memory_space=pltpu.HBM)] * len(arguments),
        out_specs=pl.BlockSpec(memory_space=pltpu.VMEM),
        scratch_shapes=[pltpu.VMEM(a.shape, a.dtype) for a in arguments]
        + [
            pltpu.VMEM((hid, inputs), bf16),
            pltpu.VMEM((hid, inputs), bf16),
            pltpu.VMEM((hid, nodes), bf16),
            pltpu.VMEM((CHUNKS, width, slots // CHUNKS), bf16),
            pltpu.VMEM((width, nodes), jnp.float32),
            pltpu.VMEM((CHUNKS, hid, slots // CHUNKS), bf16),
            pltpu.VMEM((hid, nodes), bf16),
            pltpu.VMEM((CHUNKS, cols, width, slots // CHUNKS), bf16),
            pltpu.VMEM((cols, width, nodes), bf16),
            pltpu.VMEM((nodes, slots), bf16),
            pltpu.VMEM((parts, short, LANES), bf16),
            pltpu.VMEM((parts, short, LANES), bf16),
            pltpu.VMEM((width, nodes), jnp.float32),
            pltpu.VMEM((nodes + slots, nodes), bf16),
            copies((len(arguments),)),
            copies((CHUNKS, cols - 1)),
            copies((CHUNKS, cols)),
            copies((parts,)),
            copies((parts,)),
            copies((cols - 1,)),
            copies((cols,)),
        ],
        compiler_params=pltpu.CompilerParams(
            collective_id=0, has_side_effects=True, vmem_limit_bytes=limit
        ),
        name="layer",
    )(*[pltpu.with_memory_space_constraint(a, pltpu.HBM) for a in arguments])


def solution(mesh):
    return jax.shard_map(
        local,
        mesh=mesh,
        in_specs=(
            P("cols", "dom"),
            P("cols", None),
            P(),
            P(),
            P(None, "dom"),
            P("dom"),
            P("dom", None),
            P("dom", None),
        ),
        out_specs=P("cols", "dom"),
        check_vma=False,
    )
```

```python
import functools

import jax
import jax.numpy as jnp
from jax import lax
from jax.experimental import pallas as pl
from jax.experimental.pallas import tpu as pltpu
from jax.sharding import PartitionSpec as P

MESH = pl.DeviceIdType.MESH
LANES = 128
CHUNKS = 4
NEAR = 2


def dot(left, right, left_dim, right_dim):
    return lax.dot_general(
        left, right, (((left_dim,), (right_dim,)), ((), ())), preferred_element_type=jnp.float32
    )


def partner(me, step, count):
    if count & (count - 1):
        return (me + step) % count
    other = me
    for bit in range(count.bit_length()):
        if step >> bit & 1:
            size = 1 << bit
            other = other + size - 2 * size * (me // size % 2)
    return other


def kernel(
    cols,
    parts,
    capacity,
    feat_hbm,
    proj_hbm,
    selfw_hbm,
    neighw_hbm,
    neigh_hbm,
    degree_hbm,
    rows_hbm,
    count_hbm,
    out_ref,
    feat,
    proj,
    selfw,
    neighw,
    neigh,
    degree,
    rows,
    count,
    weights,
    weights_self,
    projected,
    own,
    own_self,
    outgoing_sum,
    outgoing_self,
    incoming_sum,
    incoming_self,
    pick,
    packed_out,
    packed_in,
    remote,
    counts,
    in_sem,
    sum_send,
    sum_recv,
    row_send,
    row_recv,
    self_send,
    self_recv,
    known,
):
    column = lax.axis_index("cols")
    part = lax.axis_index("dom")
    width = out_ref.shape[0]
    nodes = out_ref.shape[1]
    slots = rows.shape[1]
    slot_count = neigh.shape[0]
    fold = LANES // capacity
    short = width // fold
    pairs = parts // fold
    steps = sorted(range(1, cols), key=lambda step: -bin(step).count("1"))

    barrier = pltpu.get_barrier_semaphore()
    for step in range(1, cols):
        pl.semaphore_signal(
            barrier, inc=1, device_id=((column + step) % cols, part), device_id_type=MESH
        )

    def aside(distance, act):
        for way, offset in enumerate((-distance, distance)):

            @pl.when((part + offset >= 0) & (part + offset < parts))
            def _():
                act(way, part + offset)

    for distance in range(1, NEAR + 1):
        aside(
            distance,
            lambda way, peer: pl.semaphore_signal(
                barrier, inc=1, device_id=(column, peer), device_id_type=MESH
            ),
        )

    def enter():
        peers = cols - 1
        for distance in range(1, NEAR + 1):
            peers = peers + (part - distance + parts) // parts + 1 - (part + distance) // parts
        pl.semaphore_wait(barrier, peers)

    def tell(stage):
        aside(
            NEAR << stage,
            lambda way, peer: pl.semaphore_signal(
                known.at[stage, 1 - way], inc=1, device_id=(column, peer), device_id_type=MESH
            ),
        )

    def hear(stage):
        aside(NEAR << stage, lambda way, peer: pl.semaphore_wait(known.at[stage, way], 1))

    stages = 0
    while NEAR << stages < parts - 1:
        stages += 1

    loads = [
        pltpu.make_async_copy(source, target, in_sem.at[i])
        for i, (source, target) in enumerate(
            (
                (rows_hbm, rows),
                (count_hbm, count),
                (feat_hbm, feat),
                (neighw_hbm, neighw),
                (proj_hbm, proj),
                (selfw_hbm, selfw),
                (neigh_hbm, neigh),
                (degree_hbm, degree),
            )
        )
    ]
    for load in loads:
        load.start()

    def band(index):
        return pl.ds(pl.multiple_of(index * width, width), width)

    def scatter(source, target, send, recv, peer):
        return pltpu.make_async_remote_copy(
            src_ref=source,
            dst_ref=target,
            send_sem=send,
            recv_sem=recv,
            device_id=(peer, part),
            device_id_type=MESH,
        )

    def sum_copy(chunk, step, arriving=False):
        peer = partner(column, step, cols)
        slot = peer if arriving else column
        return scatter(
            outgoing_sum.at[chunk, band(peer)],
            incoming_sum.at[chunk, slot],
            sum_send.at[chunk, step - 1],
            sum_recv.at[chunk, slot],
            peer,
        )

    def self_copy(step, arriving=False):
        peer = partner(column, step, cols)
        slot = peer if arriving else column
        return scatter(
            outgoing_self.at[band(peer)],
            incoming_self.at[slot],
            self_send.at[step - 1],
            self_recv.at[slot],
            peer,
        )

    lanes = slots // CHUNKS
    rate = parts // CHUNKS
    group = min(lanes, 512)

    def choose(chunk):
        amount = jnp.zeros((1, lanes), jnp.int32)
        place = lax.broadcasted_iota(jnp.int32, (1, lanes), 1)
        for index in range(rate):
            here = place // capacity == index
            peer = chunk * rate + index
            amount = jnp.where(here, count[:, peer : peer + 1], amount)
        wanted = jnp.where(
            place % capacity < amount, rows[:, chunk * lanes : (chunk + 1) * lanes], -1
        )
        for start in range(0, lanes, group):
            hit = (
                lax.broadcasted_iota(jnp.int32, (nodes, group), 0)
                == wanted[:, start : start + group]
            )
            there = slice(chunk * lanes + start, chunk * lanes + start + group)
            pick[:, there] = jnp.where(hit, 1.0, 0.0).astype(jnp.bfloat16)

    for load in loads[:5]:
        load.wait()
    turned = dot(neighw[...], proj[...], 0, 1).astype(jnp.bfloat16)
    for chunk in range(CHUNKS):
        choose(chunk)
    value = dot(turned, feat[...], 1, 0).astype(jnp.bfloat16)
    projected[...] = value
    whole = dot(value, pick[...], 1, 0).astype(jnp.bfloat16)
    for chunk in range(CHUNKS):
        outgoing_sum[chunk] = whole[:, chunk * lanes : (chunk + 1) * lanes]
    enter()
    for chunk in range(CHUNKS):
        for step in steps:
            sum_copy(chunk, step).start()
    tell(0)
    for chunk in range(CHUNKS):
        own[chunk] = outgoing_sum[chunk, band(column), :]
    for load in loads[5:]:
        load.wait()
    weights_self[...] = dot(selfw[...], proj[...], 0, 1).astype(jnp.bfloat16)
    used = lax.broadcasted_iota(jnp.int32, (slot_count, nodes), 0) < degree[...]
    codes = jnp.where(used, neigh[...], -1)
    neigh[...] = codes
    depth = 256
    row_of = lax.broadcasted_iota(jnp.int32, (depth, LANES), 0).astype(jnp.float32).astype(jnp.bfloat16)
    one = jnp.ones((depth, LANES), jnp.bfloat16)
    zero = jnp.zeros((depth, LANES), jnp.bfloat16)

    def tally(index, carry):
        start = pl.multiple_of(index * depth, depth)
        for lane in range(nodes // LANES):
            there = slice(lane * LANES, (lane + 1) * LANES)
            near = jnp.clip(neigh[:, there] - start, -1, depth).astype(jnp.float32)
            total = zero
            for slot in range(slot_count):
                code = jnp.broadcast_to(near[slot : slot + 1, :], (16, LANES)).astype(jnp.bfloat16)
                code = jnp.concatenate([code] * (depth // 16), axis=0)
                total = total + jnp.where(row_of == code, one, zero)
            counts[pl.ds(start, depth), there] = total
        return carry

    lax.fori_loop(0, nodes // depth, tally, 0)
    share = 1.0 / degree[...].astype(jnp.float32)
    value = dot(projected[...], counts[0:nodes, :], 1, 0) * share
    value = value + dot(weights_self[...], feat[...], 1, 0)
    outgoing_self[...] = value.astype(jnp.bfloat16)
    for step in steps:
        self_copy(step).start()
    own_self[...] = outgoing_self[band(column), :].astype(jnp.float32)
    if stages:
        hear(0)
    if stages > 1:
        tell(1)
    lax.fori_loop(nodes // depth, counts.shape[0] // depth, tally, 0)
    packed_in[part] = jnp.zeros((short, LANES), jnp.bfloat16)

    def part_copy(peer, slot):
        return pltpu.make_async_remote_copy(
            src_ref=packed_out.at[peer],
            dst_ref=packed_in.at[slot],
            send_sem=row_send.at[peer],
            recv_sem=row_recv.at[slot],
            device_id=(column, peer),
            device_id_type=MESH,
        )

    half = lax.broadcasted_iota(jnp.int32, (short, LANES), 1) // capacity

    for stage in range(1, stages):
        hear(stage)
        if stage + 1 < stages:
            tell(stage + 1)
    for chunk in range(CHUNKS):
        for step in steps:
            sum_copy(chunk, step, True).wait_recv()
        total = own[chunk].astype(jnp.float32)
        for step in steps:
            total = total + incoming_sum[chunk, partner(column, step, cols)].astype(jnp.float32)
        first = chunk * rate
        for place in range(rate):
            block = total[:, place // fold * LANES : (place // fold + 1) * LANES]
            tight = None
            for piece in range(fold):
                shift = (piece - place % fold) * capacity % LANES
                value = block[piece * short : (piece + 1) * short, :]
                value = pltpu.roll(value, shift, 1) if shift else value
                tight = value if tight is None else jnp.where(half == piece, value, tight)
            packed_out[first + place] = tight.astype(jnp.bfloat16)
        for place in range(rate):

            @pl.when(first + place != part)
            def _():
                part_copy(first + place, part).start()

    remote[...] = jnp.zeros((width, nodes), jnp.float32)

    def gather(turn, carry):
        pair = (part // fold + turn) % pairs
        blocks = []
        for place in range(fold):
            peer = pair * fold + place

            @pl.when(peer != part)
            def _():
                part_copy(peer, peer).wait_recv()

        for place in range(fold):
            blocks.append(packed_in[pair * fold + place].astype(jnp.float32))
        pieces = []
        for piece in range(fold):
            value = jnp.zeros((short, LANES), jnp.float32)
            for place in range(fold):
                shift = (place - piece) * capacity % LANES
                block = pltpu.roll(blocks[place], shift, 1) if shift else blocks[place]
                value = jnp.where(half == place, block, value)
            pieces.append(value)
        table = jnp.concatenate(pieces, axis=0).astype(jnp.bfloat16)
        start = pl.multiple_of(nodes + pair * LANES, LANES)
        remote[...] += dot(table, counts[pl.ds(start, LANES), :], 1, 0)
        return carry

    lax.fori_loop(0, pairs, gather, 0)
    total = own_self[...]
    for step in steps:
        self_copy(step, True).wait_recv()
    for step in steps:
        total = total + incoming_self[partner(column, step, cols)].astype(jnp.float32)
    result = total + remote[...] * share
    out_ref[...] = jnp.maximum(result, 0.0).astype(out_ref.dtype)
    for step in steps:
        for chunk in range(CHUNKS):
            sum_copy(chunk, step).wait_send()
        self_copy(step).wait_send()

    def sent(peer, carry):
        @pl.when(peer != part)
        def _():
            part_copy(peer, part).wait_send()

        return carry

    lax.fori_loop(0, parts, sent, 0)


def local(features, proj_in, self_weight, neigh_weight, neighbors, degree, send_rows, send_count):
    cols = lax.axis_size("cols")
    parts = lax.axis_size("dom")
    inputs, hid = proj_in.shape
    width = hid // cols
    nodes = features.shape[1]
    slots = send_rows.shape[1]
    capacity = slots // parts
    fold = LANES // capacity
    short = width // fold
    degree = degree.reshape(1, nodes)
    arguments = (
        features,
        proj_in,
        self_weight,
        neigh_weight,
        neighbors,
        degree,
        send_rows,
        send_count,
    )
    bf16 = jnp.bfloat16
    copies = pltpu.SemaphoreType.DMA
    limit = (16 << 20) + (slots * nodes + slots * hid + hid * nodes * 8) * 4
    return pl.pallas_call(
        functools.partial(kernel, cols, parts, capacity),
        out_shape=jax.ShapeDtypeStruct((width, nodes), bf16),
        in_specs=[pl.BlockSpec(memory_space=pltpu.HBM)] * len(arguments),
        out_specs=pl.BlockSpec(memory_space=pltpu.VMEM),
        scratch_shapes=[pltpu.VMEM(a.shape, a.dtype) for a in arguments]
        + [
            pltpu.VMEM((hid, inputs), bf16),
            pltpu.VMEM((hid, inputs), bf16),
            pltpu.VMEM((hid, nodes), bf16),
            pltpu.VMEM((CHUNKS, width, slots // CHUNKS), bf16),
            pltpu.VMEM((width, nodes), jnp.float32),
            pltpu.VMEM((CHUNKS, hid, slots // CHUNKS), bf16),
            pltpu.VMEM((hid, nodes), bf16),
            pltpu.VMEM((CHUNKS, cols, width, slots // CHUNKS), bf16),
            pltpu.VMEM((cols, width, nodes), bf16),
            pltpu.VMEM((nodes, slots), bf16),
            pltpu.VMEM((parts, short, LANES), bf16),
            pltpu.VMEM((parts, short, LANES), bf16),
            pltpu.VMEM((width, nodes), jnp.float32),
            pltpu.VMEM((nodes + slots, nodes), bf16),
            copies((len(arguments),)),
            copies((CHUNKS, cols - 1)),
            copies((CHUNKS, cols)),
            copies((parts,)),
            copies((parts,)),
            copies((cols - 1,)),
            copies((cols,)),
            pltpu.SemaphoreType.REGULAR((parts.bit_length(), 2)),
        ],
        compiler_params=pltpu.CompilerParams(
            collective_id=0, has_side_effects=True, vmem_limit_bytes=limit
        ),
        name="layer",
    )(*[pltpu.with_memory_space_constraint(a, pltpu.HBM) for a in arguments])


def solution(mesh):
    return jax.shard_map(
        local,
        mesh=mesh,
        in_specs=(
            P("cols", "dom"),
            P("cols", None),
            P(),
            P(),
            P(None, "dom"),
            P("dom"),
            P("dom", None),
            P("dom", None),
        ),
        out_specs=P("cols", "dom"),
        check_vma=False,
    )
```

```python
import functools

import jax
import jax.numpy as jnp
from jax import lax
from jax.experimental import pallas as pl
from jax.experimental.pallas import tpu as pltpu
from jax.sharding import PartitionSpec as P

MESH = pl.DeviceIdType.MESH
LANES = 128
CHUNKS = 4


def dot(left, right, left_dim, right_dim):
    return lax.dot_general(
        left, right, (((left_dim,), (right_dim,)), ((), ())), preferred_element_type=jnp.float32
    )


def partner(me, step, count):
    if count & (count - 1):
        return (me + step) % count
    other = me
    for bit in range(count.bit_length()):
        if step >> bit & 1:
            size = 1 << bit
            other = other + size - 2 * size * (me // size % 2)
    return other


def kernel(
    cols,
    parts,
    capacity,
    feat_hbm,
    proj_hbm,
    selfw_hbm,
    neighw_hbm,
    neigh_hbm,
    degree_hbm,
    rows_hbm,
    count_hbm,
    out_ref,
    feat,
    proj,
    selfw,
    neighw,
    neigh,
    degree,
    rows,
    count,
    weights,
    weights_self,
    projected,
    own_self,
    outgoing_sum,
    outgoing_self,
    incoming_sum,
    incoming_self,
    pick,
    packed_out,
    packed_in,
    remote,
    counts,
    in_sem,
    sum_send,
    sum_recv,
    row_send,
    row_recv,
    self_send,
    self_recv,
    known,
):
    column = lax.axis_index("cols")
    part = lax.axis_index("dom")
    width = out_ref.shape[0]
    nodes = out_ref.shape[1]
    slots = rows.shape[1]
    slot_count = neigh.shape[0]
    fold = LANES // capacity
    pairs = parts // fold
    pair = part // fold
    member = part % fold
    carrier = pair * fold + fold - 1
    steps = sorted(range(1, cols), key=lambda step: -bin(step).count("1"))

    loads = [
        pltpu.make_async_copy(source, target, in_sem.at[i])
        for i, (source, target) in enumerate(
            (
                (rows_hbm, rows),
                (count_hbm, count),
                (feat_hbm, feat),
                (neighw_hbm, neighw),
                (proj_hbm, proj),
                (selfw_hbm, selfw),
                (neigh_hbm, neigh),
                (degree_hbm, degree),
            )
        )
    ]
    for load in loads[:5]:
        load.start()

    barrier = pltpu.get_barrier_semaphore()

    def greet(target, place):
        pl.semaphore_signal(
            barrier, inc=1, device_id=(target, place), device_id_type=MESH
        )

    for step in range(cols):
        for turn in range(1 if step == 0 else 0, fold):
            greet((column + step) % cols, pair * fold + (part + turn) % fold)
    for way in (-1, 1):

        @pl.when((pair + way >= 0) & (pair + way < pairs))
        def _():
            for place in range(fold):
                greet(column, (pair + way) * fold + place)

    def enter():
        beside = (pair - 1 + pairs) // pairs + 1 - (pair + 1) // pairs
        pl.semaphore_wait(barrier, cols * fold - 1 + beside * fold)

    def aside(distance, act):
        for way, offset in enumerate((-distance, distance)):

            @pl.when((part + offset >= 0) & (part + offset < parts))
            def _():
                act(way, part + offset)

    def tell(stage):
        aside(
            fold << stage,
            lambda way, peer: pl.semaphore_signal(
                known.at[stage, 1 - way], inc=1, device_id=(column, peer), device_id_type=MESH
            ),
        )

    def hear(stage):
        aside(fold << stage, lambda way, peer: pl.semaphore_wait(known.at[stage, way], 1))

    stages = 0
    while 1 << stages < pairs - 1:
        stages += 1

    for load in loads[5:]:
        load.start()

    def band(index):
        return pl.ds(pl.multiple_of(index * width, width), width)

    def scatter(source, target, send, recv, peer, place):
        return pltpu.make_async_remote_copy(
            src_ref=source,
            dst_ref=target,
            send_sem=send,
            recv_sem=recv,
            device_id=(peer, place),
            device_id_type=MESH,
        )

    def sum_copy(chunk, step, place=None):
        peer = partner(column, step, cols)
        slot = column if place is None else peer
        place = member if place is None else place
        return scatter(
            outgoing_sum.at[chunk, band(peer)],
            incoming_sum.at[chunk, place, slot],
            sum_send.at[chunk, step],
            sum_recv.at[chunk, place, slot],
            peer,
            carrier,
        )

    def sum_start(chunk):
        for step in steps:
            sum_copy(chunk, step).start()

        @pl.when(part != carrier)
        def _():
            sum_copy(chunk, 0).start()

    def self_copy(step, arriving=False):
        peer = partner(column, step, cols)
        slot = peer if arriving else column
        return scatter(
            outgoing_self.at[band(peer)],
            incoming_self.at[slot],
            self_send.at[step - 1],
            self_recv.at[slot],
            peer,
            part,
        )

    lanes = slots // CHUNKS
    rate = parts // CHUNKS
    group = min(lanes, 512)

    def choose(chunk):
        amount = jnp.zeros((1, lanes), jnp.int32)
        place = lax.broadcasted_iota(jnp.int32, (1, lanes), 1)
        for index in range(rate):
            here = place // capacity == index
            peer = chunk * rate + index
            amount = jnp.where(here, count[:, peer : peer + 1], amount)
        wanted = jnp.where(
            place % capacity < amount, rows[:, chunk * lanes : (chunk + 1) * lanes], -1
        )
        for start in range(0, lanes, group):
            hit = (
                lax.broadcasted_iota(jnp.int32, (nodes, group), 0)
                == wanted[:, start : start + group]
            )
            there = slice(chunk * lanes + start, chunk * lanes + start + group)
            pick[:, there] = jnp.where(hit, 1.0, 0.0).astype(jnp.bfloat16)

    for load in loads[:5]:
        load.wait()
    choose(0)
    picked = dot(feat[...], pick[:, 0:lanes], 1, 0).astype(jnp.bfloat16)
    turned = dot(neighw[...], proj[...], 0, 1).astype(jnp.bfloat16)
    weights[...] = turned
    outgoing_sum[0] = dot(turned, picked, 1, 0).astype(jnp.bfloat16)
    enter()
    sum_start(0)
    tell(0)
    for chunk in range(1, CHUNKS):
        choose(chunk)
    value = dot(weights[...], feat[...], 1, 0).astype(jnp.bfloat16)
    projected[...] = value
    whole = dot(value, pick[:, lanes:], 1, 0).astype(jnp.bfloat16)
    for chunk in range(1, CHUNKS):
        outgoing_sum[chunk] = whole[:, (chunk - 1) * lanes : chunk * lanes]
    for chunk in range(1, CHUNKS):
        sum_start(chunk)
    for load in loads[5:]:
        load.wait()
    weights_self[...] = dot(selfw[...], proj[...], 0, 1).astype(jnp.bfloat16)
    used = lax.broadcasted_iota(jnp.int32, (slot_count, nodes), 0) < degree[...]
    codes = jnp.where(used, neigh[...], -1)
    neigh[...] = codes
    depth = 256
    row_of = lax.broadcasted_iota(jnp.int32, (depth, LANES), 0).astype(jnp.float32).astype(jnp.bfloat16)
    one = jnp.ones((depth, LANES), jnp.bfloat16)
    zero = jnp.zeros((depth, LANES), jnp.bfloat16)

    def tally(index, carry):
        start = pl.multiple_of(index * depth, depth)
        for lane in range(nodes // LANES):
            there = slice(lane * LANES, (lane + 1) * LANES)
            near = jnp.clip(neigh[:, there] - start, -1, depth).astype(jnp.float32)
            total = zero
            for slot in range(slot_count):
                code = jnp.broadcast_to(near[slot : slot + 1, :], (16, LANES)).astype(jnp.bfloat16)
                code = jnp.concatenate([code] * (depth // 16), axis=0)
                total = total + jnp.where(row_of == code, one, zero)
            counts[pl.ds(start, depth), there] = total
        return carry

    lax.fori_loop(0, nodes // depth, tally, 0)
    share = 1.0 / degree[...].astype(jnp.float32)
    value = dot(projected[...], counts[0:nodes, :], 1, 0) * share
    value = value + dot(weights_self[...], feat[...], 1, 0)
    outgoing_self[...] = value.astype(jnp.bfloat16)
    for step in steps:
        self_copy(step).start()
    own_self[...] = outgoing_self[band(column), :].astype(jnp.float32)
    if stages:
        hear(0)
    if stages > 1:
        tell(1)
    lax.fori_loop(nodes // depth, counts.shape[0] // depth, tally, 0)

    def part_copy(peer, slot):
        return pltpu.make_async_remote_copy(
            src_ref=packed_out.at[peer],
            dst_ref=packed_in.at[slot],
            send_sem=row_send.at[peer],
            recv_sem=row_recv.at[slot],
            device_id=(column, peer),
            device_id_type=MESH,
        )

    half = lax.broadcasted_iota(jnp.int32, (width, LANES), 1) // capacity

    for stage in range(1, stages):
        hear(stage)
        if stage + 1 < stages:
            tell(stage + 1)

    @pl.when(part == carrier)
    def _():
        for chunk in range(CHUNKS):
            totals = []
            for place in range(fold):
                for step in steps:
                    sum_copy(chunk, step, place).wait_recv()
                if place == fold - 1:
                    total = outgoing_sum[chunk, band(column), :].astype(jnp.float32)
                else:
                    sum_copy(chunk, 0, place).wait_recv()
                    total = incoming_sum[chunk, place, column].astype(jnp.float32)
                for step in steps:
                    value = incoming_sum[chunk, place, partner(column, step, cols)]
                    total = total + value.astype(jnp.float32)
                totals.append(total)
            first = chunk * rate
            for target in range(rate):
                there = slice(target // fold * LANES, (target // fold + 1) * LANES)
                tight = None
                for place in range(fold):
                    shift = (place - target % fold) * capacity % LANES
                    value = totals[place][:, there]
                    value = pltpu.roll(value, shift, 1) if shift else value
                    tight = value if tight is None else jnp.where(half == place, value, tight)
                packed_out[first + target] = tight.astype(jnp.bfloat16)
            for target in range(rate):

                @pl.when(first + target != part)
                def _():
                    part_copy(first + target, pair).start()

        packed_in[pair] = packed_out[part]

    remote[...] = jnp.zeros((width, nodes), jnp.float32)

    def gather(turn, carry):
        source = (pair + turn) % pairs

        @pl.when(source * fold + fold - 1 != part)
        def _():
            part_copy(part, source).wait_recv()

        start = pl.multiple_of(nodes + source * LANES, LANES)
        remote[...] += dot(packed_in[source], counts[pl.ds(start, LANES), :], 1, 0)
        return carry

    for step in steps:
        for chunk in range(CHUNKS):
            sum_copy(chunk, step).wait_send()
        self_copy(step).wait_send()

    @pl.when(part != carrier)
    def _():
        for chunk in range(CHUNKS):
            sum_copy(chunk, 0).wait_send()

    lax.fori_loop(0, pairs - 1, gather, 0)
    total = own_self[...]
    for step in steps:
        self_copy(step, True).wait_recv()
    for step in steps:
        total = total + incoming_self[partner(column, step, cols)].astype(jnp.float32)
    own_self[...] = total

    def sent(peer, carry):
        @pl.when((part == carrier) & (peer != part))
        def _():
            part_copy(peer, pair).wait_send()

        return carry

    lax.fori_loop(0, parts, sent, 0)
    gather(pairs - 1, 0)
    result = own_self[...] + remote[...] * share
    out_ref[...] = jnp.maximum(result, 0.0).astype(out_ref.dtype)


def local(features, proj_in, self_weight, neigh_weight, neighbors, degree, send_rows, send_count):
    cols = lax.axis_size("cols")
    parts = lax.axis_size("dom")
    inputs, hid = proj_in.shape
    width = hid // cols
    nodes = features.shape[1]
    slots = send_rows.shape[1]
    capacity = slots // parts
    fold = LANES // capacity
    degree = degree.reshape(1, nodes)
    arguments = (
        features,
        proj_in,
        self_weight,
        neigh_weight,
        neighbors,
        degree,
        send_rows,
        send_count,
    )
    bf16 = jnp.bfloat16
    copies = pltpu.SemaphoreType.DMA
    limit = (16 << 20) + (slots * nodes + slots * hid + hid * nodes * 8) * 4
    return pl.pallas_call(
        functools.partial(kernel, cols, parts, capacity),
        out_shape=jax.ShapeDtypeStruct((width, nodes), bf16),
        in_specs=[pl.BlockSpec(memory_space=pltpu.HBM)] * len(arguments),
        out_specs=pl.BlockSpec(memory_space=pltpu.VMEM),
        scratch_shapes=[pltpu.VMEM(a.shape, a.dtype) for a in arguments]
        + [
            pltpu.VMEM((hid, inputs), bf16),
            pltpu.VMEM((hid, inputs), bf16),
            pltpu.VMEM((hid, nodes), bf16),
            pltpu.VMEM((width, nodes), jnp.float32),
            pltpu.VMEM((CHUNKS, hid, slots // CHUNKS), bf16),
            pltpu.VMEM((hid, nodes), bf16),
            pltpu.VMEM((CHUNKS, fold, cols, width, slots // CHUNKS), bf16),
            pltpu.VMEM((cols, width, nodes), bf16),
            pltpu.VMEM((nodes, slots), bf16),
            pltpu.VMEM((parts, width, LANES), bf16),
            pltpu.VMEM((parts // fold, width, LANES), bf16),
            pltpu.VMEM((width, nodes), jnp.float32),
            pltpu.VMEM((nodes + slots, nodes), bf16),
            copies((len(arguments),)),
            copies((CHUNKS, cols)),
            copies((CHUNKS, fold, cols)),
            copies((parts,)),
            copies((parts // fold,)),
            copies((cols - 1,)),
            copies((cols,)),
            pltpu.SemaphoreType.REGULAR((parts.bit_length(), 2)),
        ],
        compiler_params=pltpu.CompilerParams(
            collective_id=0, has_side_effects=True, vmem_limit_bytes=limit
        ),
        name="layer",
    )(*[pltpu.with_memory_space_constraint(a, pltpu.HBM) for a in arguments])


def solution(mesh):
    return jax.shard_map(
        local,
        mesh=mesh,
        in_specs=(
            P("cols", "dom"),
            P("cols", None),
            P(),
            P(),
            P(None, "dom"),
            P("dom"),
            P("dom", None),
            P("dom", None),
        ),
        out_specs=P("cols", "dom"),
        check_vma=False,
    )
```

```python
import functools

import jax
import jax.numpy as jnp
from jax import lax
from jax.experimental import pallas as pl
from jax.experimental.pallas import tpu as pltpu
from jax.sharding import PartitionSpec as P

MESH = pl.DeviceIdType.MESH
LANES = 128
CHUNKS = 4


def dot(left, right, left_dim, right_dim):
    return lax.dot_general(
        left, right, (((left_dim,), (right_dim,)), ((), ())), preferred_element_type=jnp.float32
    )


def partner(me, step, count):
    if count & (count - 1):
        return (me + step) % count
    other = me
    for bit in range(count.bit_length()):
        if step >> bit & 1:
            size = 1 << bit
            other = other + size - 2 * size * (me // size % 2)
    return other


def rounds(pairs):
    stages = 0
    while 1 << stages < pairs - 1:
        stages += 1
    return stages


def kernel(
    cols,
    parts,
    capacity,
    feat_hbm,
    proj_hbm,
    selfw_hbm,
    neighw_hbm,
    neigh_hbm,
    degree_hbm,
    rows_hbm,
    count_hbm,
    out_ref,
    feat,
    proj,
    selfw,
    neighw,
    neigh,
    degree,
    rows,
    count,
    weights,
    weights_self,
    projected,
    own_self,
    outgoing_sum,
    outgoing_self,
    incoming_sum,
    incoming_self,
    pick,
    packed_out,
    packed_in,
    remote,
    counts,
    in_sem,
    sends,
    sum_recv,
    row_recv,
    self_recv,
    known,
):
    column = lax.axis_index("cols")
    part = lax.axis_index("dom")
    width = out_ref.shape[0]
    nodes = out_ref.shape[1]
    slots = rows.shape[1]
    slot_count = neigh.shape[0]
    fold = LANES // capacity
    pairs = parts // fold
    pair = part // fold
    member = part % fold
    carrier = pair * fold + fold - 1
    steps = sorted(range(1, cols), key=lambda step: -bin(step).count("1"))

    loads = [
        pltpu.make_async_copy(source, target, in_sem.at[i])
        for i, (source, target) in enumerate(
            (
                (rows_hbm, rows),
                (count_hbm, count),
                (feat_hbm, feat),
                (neighw_hbm, neighw),
                (proj_hbm, proj),
                (selfw_hbm, selfw),
                (neigh_hbm, neigh),
                (degree_hbm, degree),
            )
        )
    ]
    for load in loads[:5]:
        load.start()

    barrier = pltpu.get_barrier_semaphore()

    def greet(target, place):
        pl.semaphore_signal(
            barrier, inc=1, device_id=(target, place), device_id_type=MESH
        )

    for step in range(cols):
        for turn in range(1 if step == 0 else 0, fold):
            greet((column + step) % cols, pair * fold + (part + turn) % fold)
    for way in (-1, 1):

        @pl.when((pair + way >= 0) & (pair + way < pairs))
        def _():
            for place in range(fold):
                greet(column, (pair + way) * fold + place)

    def enter():
        beside = (pair - 1 + pairs) // pairs + 1 - (pair + 1) // pairs
        pl.semaphore_wait(barrier, cols * fold - 1 + beside * fold)

    def aside(distance, act):
        for way, offset in enumerate((-distance, distance)):

            @pl.when((part + offset >= 0) & (part + offset < parts))
            def _():
                act(way, part + offset)

    def tell(stage):
        aside(
            fold << stage,
            lambda way, peer: pl.semaphore_signal(
                known.at[stage, 1 - way], inc=1, device_id=(column, peer), device_id_type=MESH
            ),
        )

    def hear(stage):
        aside(fold << stage, lambda way, peer: pl.semaphore_wait(known.at[stage, way], 1))

    stages = rounds(pairs)

    for load in loads[5:]:
        load.start()

    def band(index):
        return pl.ds(pl.multiple_of(index * width, width), width)

    def scatter(source, target, send, recv, peer, place):
        return pltpu.make_async_remote_copy(
            src_ref=source,
            dst_ref=target,
            send_sem=send,
            recv_sem=recv,
            device_id=(peer, place),
            device_id_type=MESH,
        )

    def sum_copy(chunk, step):
        peer = partner(column, step, cols)
        return scatter(
            outgoing_sum.at[chunk, band(peer)],
            incoming_sum.at[chunk, member * cols + column],
            sends.at[0],
            sum_recv.at[chunk],
            peer,
            carrier,
        )

    def settle(refs, semaphore):
        pltpu.make_async_copy(refs, refs, semaphore).wait()

    def sum_start(chunk):
        for step in steps:
            sum_copy(chunk, step).start()

        @pl.when(part != carrier)
        def _():
            sum_copy(chunk, 0).start()

    def self_copy(step):
        peer = partner(column, step, cols)
        return scatter(
            outgoing_self.at[band(peer)],
            incoming_self.at[column],
            sends.at[1],
            self_recv.at[0],
            peer,
            part,
        )

    lanes = slots // CHUNKS
    rate = parts // CHUNKS
    group = min(lanes, 512)

    def choose(chunk):
        amount = jnp.zeros((1, lanes), jnp.int32)
        place = lax.broadcasted_iota(jnp.int32, (1, lanes), 1)
        for index in range(rate):
            here = place // capacity == index
            peer = chunk * rate + index
            amount = jnp.where(here, count[:, peer : peer + 1], amount)
        wanted = jnp.where(
            place % capacity < amount, rows[:, chunk * lanes : (chunk + 1) * lanes], -1
        )
        for start in range(0, lanes, group):
            hit = (
                lax.broadcasted_iota(jnp.int32, (nodes, group), 0)
                == wanted[:, start : start + group]
            )
            there = slice(chunk * lanes + start, chunk * lanes + start + group)
            pick[:, there] = jnp.where(hit, 1.0, 0.0).astype(jnp.bfloat16)

    for load in loads[:5]:
        load.wait()
    choose(0)
    picked = dot(feat[...], pick[:, 0:lanes], 1, 0).astype(jnp.bfloat16)
    turned = dot(neighw[...], proj[...], 0, 1).astype(jnp.bfloat16)
    weights[...] = turned
    outgoing_sum[0] = dot(turned, picked, 1, 0).astype(jnp.bfloat16)
    enter()
    sum_start(0)
    tell(0)
    for chunk in range(1, CHUNKS):
        choose(chunk)
    value = dot(weights[...], feat[...], 1, 0).astype(jnp.bfloat16)
    projected[...] = value
    whole = dot(value, pick[:, lanes:], 1, 0).astype(jnp.bfloat16)
    for chunk in range(1, CHUNKS):
        outgoing_sum[chunk] = whole[:, (chunk - 1) * lanes : chunk * lanes]
    for chunk in range(1, CHUNKS):
        sum_start(chunk)
    for load in loads[5:]:
        load.wait()
    weights_self[...] = dot(selfw[...], proj[...], 0, 1).astype(jnp.bfloat16)
    used = lax.broadcasted_iota(jnp.int32, (slot_count, nodes), 0) < degree[...]
    codes = jnp.where(used, neigh[...], -1)
    neigh[...] = codes
    depth = 256
    row_of = lax.broadcasted_iota(jnp.int32, (depth, LANES), 0).astype(jnp.float32).astype(jnp.bfloat16)
    one = jnp.ones((depth, LANES), jnp.bfloat16)
    zero = jnp.zeros((depth, LANES), jnp.bfloat16)

    def tally(index, carry):
        start = pl.multiple_of(index * depth, depth)
        for lane in range(nodes // LANES):
            there = slice(lane * LANES, (lane + 1) * LANES)
            near = jnp.clip(neigh[:, there] - start, -1, depth).astype(jnp.float32)
            total = zero
            for slot in range(slot_count):
                code = jnp.broadcast_to(near[slot : slot + 1, :], (16, LANES)).astype(jnp.bfloat16)
                code = jnp.concatenate([code] * (depth // 16), axis=0)
                total = total + jnp.where(row_of == code, one, zero)
            counts[pl.ds(start, depth), there] = total
        return carry

    lax.fori_loop(0, nodes // depth, tally, 0)
    share = 1.0 / degree[...].astype(jnp.float32)
    value = dot(projected[...], counts[0:nodes, :], 1, 0) * share
    value = value + dot(weights_self[...], feat[...], 1, 0)
    outgoing_self[...] = value.astype(jnp.bfloat16)
    for step in steps:
        self_copy(step).start()
    own_self[...] = outgoing_self[band(column), :].astype(jnp.float32)
    if stages:
        hear(0)
    if stages > 1:
        tell(1)
    lax.fori_loop(nodes // depth, counts.shape[0] // depth, tally, 0)

    def part_copy(peer, slot):
        return pltpu.make_async_remote_copy(
            src_ref=packed_out.at[peer],
            dst_ref=packed_in.at[slot],
            send_sem=sends.at[2],
            recv_sem=row_recv.at[slot],
            device_id=(column, peer),
            device_id_type=MESH,
        )

    half = lax.broadcasted_iota(jnp.int32, (width, LANES), 1) // capacity

    for stage in range(1, stages):
        hear(stage)
        if stage + 1 < stages:
            tell(stage + 1)

    @pl.when(part == carrier)
    def _():
        for chunk in range(CHUNKS):
            settle(incoming_sum.at[chunk, pl.ds(0, fold * cols - 1)], sum_recv.at[chunk])
            totals = []
            for place in range(fold):
                if place == fold - 1:
                    total = outgoing_sum[chunk, band(column), :].astype(jnp.float32)
                else:
                    total = incoming_sum[chunk, place * cols + column].astype(jnp.float32)
                for step in steps:
                    value = incoming_sum[chunk, place * cols + partner(column, step, cols)]
                    total = total + value.astype(jnp.float32)
                totals.append(total)
            first = chunk * rate
            for target in range(rate):
                there = slice(target // fold * LANES, (target // fold + 1) * LANES)
                tight = None
                for place in range(fold):
                    shift = (place - target % fold) * capacity % LANES
                    value = totals[place][:, there]
                    value = pltpu.roll(value, shift, 1) if shift else value
                    tight = value if tight is None else jnp.where(half == place, value, tight)
                packed_out[first + target] = tight.astype(jnp.bfloat16)
            for target in range(rate):

                @pl.when(first + target != part)
                def _():
                    part_copy(first + target, pair).start()

        packed_in[pair] = packed_out[part]

    remote[...] = jnp.zeros((width, nodes), jnp.float32)

    def gather(turn, carry):
        source = (pair + turn) % pairs

        @pl.when(source * fold + fold - 1 != part)
        def _():
            part_copy(part, source).wait_recv()

        start = pl.multiple_of(nodes + source * LANES, LANES)
        remote[...] += dot(packed_in[source], counts[pl.ds(start, LANES), :], 1, 0)
        return carry

    lax.fori_loop(0, pairs - 1, gather, 0)
    total = own_self[...]
    settle(incoming_self.at[pl.ds(0, cols - 1)], self_recv.at[0])
    for step in steps:
        total = total + incoming_self[partner(column, step, cols)].astype(jnp.float32)
    own_self[...] = total

    settle(outgoing_self.at[pl.ds(0, (cols - 1) * width)], sends.at[1])

    @pl.when(part == carrier)
    def _():
        settle(outgoing_sum.at[:, pl.ds(0, (cols - 1) * width)], sends.at[0])
        settle(packed_out.at[pl.ds(0, parts - 1)], sends.at[2])

    @pl.when(part != carrier)
    def _():
        settle(outgoing_sum, sends.at[0])

    gather(pairs - 1, 0)
    result = own_self[...] + remote[...] * share
    out_ref[...] = jnp.maximum(result, 0.0).astype(out_ref.dtype)


def local(features, proj_in, self_weight, neigh_weight, neighbors, degree, send_rows, send_count):
    cols = lax.axis_size("cols")
    parts = lax.axis_size("dom")
    inputs, hid = proj_in.shape
    width = hid // cols
    nodes = features.shape[1]
    slots = send_rows.shape[1]
    capacity = slots // parts
    fold = LANES // capacity
    degree = degree.reshape(1, nodes)
    arguments = (
        features,
        proj_in,
        self_weight,
        neigh_weight,
        neighbors,
        degree,
        send_rows,
        send_count,
    )
    bf16 = jnp.bfloat16
    copies = pltpu.SemaphoreType.DMA
    limit = (16 << 20) + (slots * nodes + slots * hid + hid * nodes * 8) * 4
    return pl.pallas_call(
        functools.partial(kernel, cols, parts, capacity),
        out_shape=jax.ShapeDtypeStruct((width, nodes), bf16),
        in_specs=[pl.BlockSpec(memory_space=pltpu.HBM)] * len(arguments),
        out_specs=pl.BlockSpec(memory_space=pltpu.VMEM),
        scratch_shapes=[pltpu.VMEM(a.shape, a.dtype) for a in arguments]
        + [
            pltpu.VMEM((hid, inputs), bf16),
            pltpu.VMEM((hid, inputs), bf16),
            pltpu.VMEM((hid, nodes), bf16),
            pltpu.VMEM((width, nodes), jnp.float32),
            pltpu.VMEM((CHUNKS, hid, slots // CHUNKS), bf16),
            pltpu.VMEM((hid, nodes), bf16),
            pltpu.VMEM((CHUNKS, fold * cols, width, slots // CHUNKS), bf16),
            pltpu.VMEM((cols, width, nodes), bf16),
            pltpu.VMEM((nodes, slots), bf16),
            pltpu.VMEM((parts, width, LANES), bf16),
            pltpu.VMEM((parts // fold, width, LANES), bf16),
            pltpu.VMEM((width, nodes), jnp.float32),
            pltpu.VMEM((nodes + slots, nodes), bf16),
            copies((len(arguments),)),
            copies((3,)),
            copies((CHUNKS,)),
            copies((parts // fold,)),
            copies((1,)),
            pltpu.SemaphoreType.REGULAR((max(1, rounds(parts // fold)), 2)),
        ],
        compiler_params=pltpu.CompilerParams(
            collective_id=0, has_side_effects=True, vmem_limit_bytes=limit
        ),
        name="layer",
    )(*[pltpu.with_memory_space_constraint(a, pltpu.HBM) for a in arguments])


def solution(mesh):
    return jax.shard_map(
        local,
        mesh=mesh,
        in_specs=(
            P("cols", "dom"),
            P("cols", None),
            P(),
            P(),
            P(None, "dom"),
            P("dom"),
            P("dom", None),
            P("dom", None),
        ),
        out_specs=P("cols", "dom"),
        check_vma=False,
    )
```

```python
import functools

import jax
import jax.numpy as jnp
from jax import lax
from jax.experimental import pallas as pl
from jax.experimental.pallas import tpu as pltpu
from jax.sharding import PartitionSpec as P

MESH = pl.DeviceIdType.MESH
LANES = 128
CHUNKS = 4


def dot(left, right, left_dim, right_dim):
    return lax.dot_general(
        left, right, (((left_dim,), (right_dim,)), ((), ())), preferred_element_type=jnp.float32
    )


def partner(me, step, count):
    if count & (count - 1):
        return (me + step) % count
    other = me
    for bit in range(count.bit_length()):
        if step >> bit & 1:
            size = 1 << bit
            other = other + size - 2 * size * (me // size % 2)
    return other


def rounds(pairs):
    stages = 0
    while 1 << stages < pairs - 1:
        stages += 1
    return stages


def kernel(
    cols,
    parts,
    capacity,
    feat_hbm,
    proj_hbm,
    selfw_hbm,
    neighw_hbm,
    neigh_hbm,
    degree_hbm,
    rows_hbm,
    count_hbm,
    out_ref,
    feat,
    proj,
    selfw,
    neighw,
    neigh,
    degree,
    rows,
    count,
    weights,
    weights_self,
    projected,
    own_self,
    outgoing_sum,
    outgoing_self,
    incoming_sum,
    incoming_self,
    pick,
    packed_out,
    packed_in,
    remote,
    counts,
    in_sem,
    sends,
    sum_recv,
    row_recv,
    self_recv,
    known,
):
    column = lax.axis_index("cols")
    part = lax.axis_index("dom")
    width = out_ref.shape[0]
    nodes = out_ref.shape[1]
    slots = rows.shape[1]
    slot_count = neigh.shape[0]
    fold = LANES // capacity
    pairs = parts // fold
    pair = part // fold
    member = part % fold
    carrier = pair * fold + fold - 1
    steps = sorted(range(1, cols), key=lambda step: -bin(step).count("1"))

    loads = [
        pltpu.make_async_copy(source, target, in_sem.at[i])
        for i, (source, target) in enumerate(
            (
                (rows_hbm, rows),
                (count_hbm, count),
                (feat_hbm, feat),
                (neighw_hbm, neighw),
                (proj_hbm, proj),
                (selfw_hbm, selfw),
                (neigh_hbm, neigh),
                (degree_hbm, degree),
            )
        )
    ]
    for load in loads[:5]:
        load.start()

    barrier = pltpu.get_barrier_semaphore()

    def greet(target, place):
        pl.semaphore_signal(
            barrier, inc=1, device_id=(target, place), device_id_type=MESH
        )

    for step in range(cols):
        for turn in range(1 if step == 0 else 0, fold):
            greet((column + step) % cols, pair * fold + (part + turn) % fold)
    for way in (-1, 1):

        @pl.when((pair + way >= 0) & (pair + way < pairs))
        def _():
            for place in range(fold):
                greet(column, (pair + way) * fold + place)

    def enter():
        beside = (pair - 1 + pairs) // pairs + 1 - (pair + 1) // pairs
        pl.semaphore_wait(barrier, cols * fold - 1 + beside * fold)

    def aside(distance, act):
        for way, offset in enumerate((-distance, distance)):

            @pl.when((part + offset >= 0) & (part + offset < parts))
            def _():
                act(way, part + offset)

    def tell(stage):
        aside(
            fold << stage,
            lambda way, peer: pl.semaphore_signal(
                known.at[stage], inc=1, device_id=(column, peer), device_id_type=MESH
            ),
        )

    def hear(stage):
        distance = fold << stage
        sides = (part - distance + parts) // parts + 1 - (part + distance) // parts
        pl.semaphore_wait(known.at[stage], sides)

    stages = rounds(pairs)

    for load in loads[5:]:
        load.start()

    def band(index):
        return pl.ds(pl.multiple_of(index * width, width), width)

    def scatter(source, target, send, recv, peer, place):
        return pltpu.make_async_remote_copy(
            src_ref=source,
            dst_ref=target,
            send_sem=send,
            recv_sem=recv,
            device_id=(peer, place),
            device_id_type=MESH,
        )

    def sum_copy(chunk, step):
        peer = partner(column, step, cols)
        return scatter(
            outgoing_sum.at[chunk, band(peer)],
            incoming_sum.at[chunk, member * cols + column],
            sends.at[0],
            sum_recv.at[chunk],
            peer,
            carrier,
        )

    def settle(refs, semaphore):
        pltpu.make_async_copy(refs, refs, semaphore).wait()

    def sum_start(chunk):
        for step in steps:
            sum_copy(chunk, step).start()

        @pl.when(part != carrier)
        def _():
            sum_copy(chunk, 0).start()

    def self_copy(step):
        peer = partner(column, step, cols)
        return scatter(
            outgoing_self.at[band(peer)],
            incoming_self.at[column],
            sends.at[0],
            self_recv.at[0],
            peer,
            part,
        )

    lanes = slots // CHUNKS
    rate = parts // CHUNKS
    group = min(lanes, 512)

    def choose(chunk):
        amount = jnp.zeros((1, lanes), jnp.int32)
        place = lax.broadcasted_iota(jnp.int32, (1, lanes), 1)
        for index in range(rate):
            here = place // capacity == index
            peer = chunk * rate + index
            amount = jnp.where(here, count[:, peer : peer + 1], amount)
        wanted = jnp.where(
            place % capacity < amount, rows[:, chunk * lanes : (chunk + 1) * lanes], -1
        )
        for start in range(0, lanes, group):
            hit = (
                lax.broadcasted_iota(jnp.int32, (nodes, group), 0)
                == wanted[:, start : start + group]
            )
            there = slice(chunk * lanes + start, chunk * lanes + start + group)
            pick[:, there] = jnp.where(hit, 1.0, 0.0).astype(jnp.bfloat16)

    for load in loads[:5]:
        load.wait()
    choose(0)
    picked = dot(feat[...], pick[:, 0:lanes], 1, 0).astype(jnp.bfloat16)
    turned = dot(neighw[...], proj[...], 0, 1).astype(jnp.bfloat16)
    weights[...] = turned
    outgoing_sum[0] = dot(turned, picked, 1, 0).astype(jnp.bfloat16)
    enter()
    sum_start(0)
    tell(0)
    for chunk in range(1, CHUNKS):
        choose(chunk)
    value = dot(weights[...], feat[...], 1, 0).astype(jnp.bfloat16)
    projected[...] = value
    whole = dot(value, pick[:, lanes:], 1, 0).astype(jnp.bfloat16)
    for chunk in range(1, CHUNKS):
        outgoing_sum[chunk] = whole[:, (chunk - 1) * lanes : chunk * lanes]
    for chunk in range(1, CHUNKS):
        sum_start(chunk)
    for load in loads[5:]:
        load.wait()
    weights_self[...] = dot(selfw[...], proj[...], 0, 1).astype(jnp.bfloat16)
    used = lax.broadcasted_iota(jnp.int32, (slot_count, nodes), 0) < degree[...]
    codes = jnp.where(used, neigh[...], -1)
    neigh[...] = codes
    depth = 256
    row_of = lax.broadcasted_iota(jnp.int32, (depth, LANES), 0).astype(jnp.float32).astype(jnp.bfloat16)
    one = jnp.ones((depth, LANES), jnp.bfloat16)
    zero = jnp.zeros((depth, LANES), jnp.bfloat16)

    def tally(index, carry):
        start = pl.multiple_of(index * depth, depth)
        for lane in range(nodes // LANES):
            there = slice(lane * LANES, (lane + 1) * LANES)
            near = jnp.clip(neigh[:, there] - start, -1, depth).astype(jnp.float32)
            total = zero
            for slot in range(slot_count):
                code = jnp.broadcast_to(near[slot : slot + 1, :], (16, LANES)).astype(jnp.bfloat16)
                code = jnp.concatenate([code] * (depth // 16), axis=0)
                total = total + jnp.where(row_of == code, one, zero)
            counts[pl.ds(start, depth), there] = total
        return carry

    lax.fori_loop(0, nodes // depth, tally, 0)
    share = 1.0 / degree[...].astype(jnp.float32)
    value = dot(projected[...], counts[0:nodes, :], 1, 0) * share
    value = value + dot(weights_self[...], feat[...], 1, 0)
    outgoing_self[...] = value.astype(jnp.bfloat16)
    for step in steps:
        self_copy(step).start()
    own_self[...] = outgoing_self[band(column), :].astype(jnp.float32)
    if stages:
        hear(0)
    if stages > 1:
        tell(1)

    def part_copy(peer, slot):
        return pltpu.make_async_remote_copy(
            src_ref=packed_out.at[peer],
            dst_ref=packed_in.at[slot],
            send_sem=sends.at[0],
            recv_sem=row_recv.at[slot],
            device_id=(column, peer),
            device_id_type=MESH,
        )

    half = lax.broadcasted_iota(jnp.int32, (width, LANES), 1) // capacity

    for stage in range(1, stages):
        hear(stage)
        if stage + 1 < stages:
            tell(stage + 1)

    @pl.when(part == carrier)
    def _():
        for chunk in range(CHUNKS):
            settle(incoming_sum.at[chunk, pl.ds(0, fold * cols - 1)], sum_recv.at[chunk])
            totals = []
            for place in range(fold):
                if place == fold - 1:
                    total = outgoing_sum[chunk, band(column), :].astype(jnp.float32)
                else:
                    total = incoming_sum[chunk, place * cols + column].astype(jnp.float32)
                for step in steps:
                    value = incoming_sum[chunk, place * cols + partner(column, step, cols)]
                    total = total + value.astype(jnp.float32)
                totals.append(total)
            first = chunk * rate
            for target in range(rate):
                there = slice(target // fold * LANES, (target // fold + 1) * LANES)
                tight = None
                for place in range(fold):
                    shift = (place - target % fold) * capacity % LANES
                    value = totals[place][:, there]
                    value = pltpu.roll(value, shift, 1) if shift else value
                    tight = value if tight is None else jnp.where(half == place, value, tight)
                packed_out[first + target] = tight.astype(jnp.bfloat16)
            for target in range(rate):

                @pl.when(first + target != part)
                def _():
                    part_copy(first + target, pair).start()

        packed_in[pair] = packed_out[part]

    lax.fori_loop(nodes // depth, counts.shape[0] // depth, tally, 0)
    remote[...] = jnp.zeros((width, nodes), jnp.float32)

    def gather(turn, carry):
        source = (pair + turn) % pairs

        @pl.when(source * fold + fold - 1 != part)
        def _():
            part_copy(part, source).wait_recv()

        start = pl.multiple_of(nodes + source * LANES, LANES)
        remote[...] += dot(packed_in[source], counts[pl.ds(start, LANES), :], 1, 0)
        return carry

    lax.fori_loop(0, pairs - 1, gather, 0)
    total = own_self[...]
    settle(incoming_self.at[pl.ds(0, cols - 1)], self_recv.at[0])
    for step in steps:
        total = total + incoming_self[partner(column, step, cols)].astype(jnp.float32)
    own_self[...] = total

    all_sums = cols * width * slots + (cols - 1) * width * nodes
    carried = all_sums - width * slots + (parts - 1) * width * LANES

    @pl.when(part == carrier)
    def _():
        settle(counts.at[pl.ds(0, carried // nodes)], sends.at[0])

    @pl.when(part != carrier)
    def _():
        settle(counts.at[pl.ds(0, all_sums // nodes)], sends.at[0])

    gather(pairs - 1, 0)
    result = own_self[...] + remote[...] * share
    out_ref[...] = jnp.maximum(result, 0.0).astype(out_ref.dtype)


def local(features, proj_in, self_weight, neigh_weight, neighbors, degree, send_rows, send_count):
    cols = lax.axis_size("cols")
    parts = lax.axis_size("dom")
    inputs, hid = proj_in.shape
    width = hid // cols
    nodes = features.shape[1]
    slots = send_rows.shape[1]
    capacity = slots // parts
    fold = LANES // capacity
    degree = degree.reshape(1, nodes)
    arguments = (
        features,
        proj_in,
        self_weight,
        neigh_weight,
        neighbors,
        degree,
        send_rows,
        send_count,
    )
    bf16 = jnp.bfloat16
    copies = pltpu.SemaphoreType.DMA
    limit = (16 << 20) + (slots * nodes + slots * hid + hid * nodes * 8) * 4
    return pl.pallas_call(
        functools.partial(kernel, cols, parts, capacity),
        out_shape=jax.ShapeDtypeStruct((width, nodes), bf16),
        in_specs=[pl.BlockSpec(memory_space=pltpu.HBM)] * len(arguments),
        out_specs=pl.BlockSpec(memory_space=pltpu.VMEM),
        scratch_shapes=[pltpu.VMEM(a.shape, a.dtype) for a in arguments]
        + [
            pltpu.VMEM((hid, inputs), bf16),
            pltpu.VMEM((hid, inputs), bf16),
            pltpu.VMEM((hid, nodes), bf16),
            pltpu.VMEM((width, nodes), jnp.float32),
            pltpu.VMEM((CHUNKS, hid, slots // CHUNKS), bf16),
            pltpu.VMEM((hid, nodes), bf16),
            pltpu.VMEM((CHUNKS, fold * cols, width, slots // CHUNKS), bf16),
            pltpu.VMEM((cols, width, nodes), bf16),
            pltpu.VMEM((nodes, slots), bf16),
            pltpu.VMEM((parts, width, LANES), bf16),
            pltpu.VMEM((parts // fold, width, LANES), bf16),
            pltpu.VMEM((width, nodes), jnp.float32),
            pltpu.VMEM((nodes + slots, nodes), bf16),
            copies((len(arguments),)),
            copies((1,)),
            copies((CHUNKS,)),
            copies((parts // fold,)),
            copies((1,)),
            pltpu.SemaphoreType.REGULAR((max(1, rounds(parts // fold)),)),
        ],
        compiler_params=pltpu.CompilerParams(
            collective_id=0, has_side_effects=True, vmem_limit_bytes=limit
        ),
        name="layer",
    )(*[pltpu.with_memory_space_constraint(a, pltpu.HBM) for a in arguments])


def solution(mesh):
    return jax.shard_map(
        local,
        mesh=mesh,
        in_specs=(
            P("cols", "dom"),
            P("cols", None),
            P(),
            P(),
            P(None, "dom"),
            P("dom"),
            P("dom", None),
            P("dom", None),
        ),
        out_specs=P("cols", "dom"),
        check_vma=False,
    )
```

```python
import functools

import jax
import jax.numpy as jnp
from jax import lax
from jax.experimental import pallas as pl
from jax.experimental.pallas import tpu as pltpu
from jax.sharding import PartitionSpec as P

MESH = pl.DeviceIdType.MESH
LANES = 128
CHUNKS = 4


def dot(left, right, left_dim, right_dim):
    return lax.dot_general(
        left, right, (((left_dim,), (right_dim,)), ((), ())), preferred_element_type=jnp.float32
    )


def partner(me, step, count):
    if count & (count - 1):
        return (me + step) % count
    other = me
    for bit in range(count.bit_length()):
        if step >> bit & 1:
            size = 1 << bit
            other = other + size - 2 * size * (me // size % 2)
    return other


def rounds(pairs):
    stages = 0
    while 1 << stages < pairs - 1:
        stages += 1
    return stages


def kernel(
    cols,
    parts,
    capacity,
    feat_hbm,
    proj_hbm,
    selfw_hbm,
    neighw_hbm,
    neigh_hbm,
    degree_hbm,
    rows_hbm,
    count_hbm,
    out_ref,
    feat,
    proj,
    selfw,
    neighw,
    neigh,
    degree,
    rows,
    count,
    weights,
    weights_self,
    projected,
    own_self,
    outgoing_sum,
    outgoing_self,
    incoming_sum,
    incoming_self,
    pick,
    packed_out,
    packed_in,
    remote,
    counts,
    in_sem,
    sends,
    sum_recv,
    row_recv,
    self_recv,
    known,
):
    column = lax.axis_index("cols")
    part = lax.axis_index("dom")
    width = out_ref.shape[0]
    nodes = out_ref.shape[1]
    slots = rows.shape[1]
    slot_count = neigh.shape[0]
    fold = LANES // capacity
    pairs = parts // fold
    pair = part // fold
    member = part % fold
    carrier = pair * fold + fold - 1
    steps = sorted(range(1, cols), key=lambda step: -bin(step).count("1"))

    loads = [
        pltpu.make_async_copy(source, target, in_sem.at[i])
        for i, (source, target) in enumerate(
            (
                (rows_hbm, rows),
                (count_hbm, count),
                (feat_hbm, feat),
                (neighw_hbm, neighw),
                (proj_hbm, proj),
                (selfw_hbm, selfw),
                (neigh_hbm, neigh),
                (degree_hbm, degree),
            )
        )
    ]
    for load in loads[:5]:
        load.start()

    barrier = pltpu.get_barrier_semaphore()

    def greet(target, place):
        pl.semaphore_signal(
            barrier, inc=1, device_id=(target, place), device_id_type=MESH
        )

    for step in range(cols):
        for turn in range(1 if step == 0 else 0, fold):
            greet((column + step) % cols, pair * fold + (part + turn) % fold)
    for way in (-1, 1):

        @pl.when((pair + way >= 0) & (pair + way < pairs))
        def _():
            for place in range(fold):
                greet(column, (pair + way) * fold + place)

    def enter():
        beside = (pair - 1 + pairs) // pairs + 1 - (pair + 1) // pairs
        pl.semaphore_wait(barrier, cols * fold - 1 + beside * fold)

    def aside(distance, act):
        for way, offset in enumerate((-distance, distance)):

            @pl.when((part + offset >= 0) & (part + offset < parts))
            def _():
                act(way, part + offset)

    def tell(stage):
        aside(
            fold << stage,
            lambda way, peer: pl.semaphore_signal(
                known.at[stage], inc=1, device_id=(column, peer), device_id_type=MESH
            ),
        )

    def hear(stage):
        distance = fold << stage
        sides = (part - distance + parts) // parts + 1 - (part + distance) // parts
        pl.semaphore_wait(known.at[stage], sides)

    stages = rounds(pairs)

    for load in loads[5:]:
        load.start()

    def band(index):
        return pl.ds(pl.multiple_of(index * width, width), width)

    def scatter(source, target, send, recv, peer, place):
        return pltpu.make_async_remote_copy(
            src_ref=source,
            dst_ref=target,
            send_sem=send,
            recv_sem=recv,
            device_id=(peer, place),
            device_id_type=MESH,
        )

    def sum_copy(chunk, step):
        peer = partner(column, step, cols)
        return scatter(
            outgoing_sum.at[chunk, band(peer)],
            incoming_sum.at[chunk, member * cols + column],
            sends.at[0],
            sum_recv.at[chunk],
            peer,
            carrier,
        )

    def settle(refs, semaphore):
        pltpu.make_async_copy(refs, refs, semaphore).wait()

    def sum_start(chunk):
        for step in steps:
            sum_copy(chunk, step).start()

        @pl.when(part != carrier)
        def _():
            sum_copy(chunk, 0).start()

    def self_copy(step):
        peer = partner(column, step, cols)
        return scatter(
            outgoing_self.at[band(peer)],
            incoming_self.at[column],
            sends.at[0],
            self_recv.at[0],
            peer,
            part,
        )

    lanes = slots // CHUNKS
    rate = parts // CHUNKS
    group = min(lanes, 512)

    def choose(chunk):
        amount = jnp.zeros((1, lanes), jnp.int32)
        place = lax.broadcasted_iota(jnp.int32, (1, lanes), 1)
        for index in range(rate):
            here = place // capacity == index
            peer = chunk * rate + index
            amount = jnp.where(here, count[:, peer : peer + 1], amount)
        wanted = jnp.where(
            place % capacity < amount, rows[:, chunk * lanes : (chunk + 1) * lanes], -1
        )
        for start in range(0, lanes, group):
            hit = (
                lax.broadcasted_iota(jnp.int32, (nodes, group), 0)
                == wanted[:, start : start + group]
            )
            there = slice(chunk * lanes + start, chunk * lanes + start + group)
            pick[:, there] = jnp.where(hit, 1.0, 0.0).astype(jnp.bfloat16)

    for load in loads[:5]:
        load.wait()
    choose(0)
    picked = dot(feat[...], pick[:, 0:lanes], 1, 0).astype(jnp.bfloat16)
    turned = dot(neighw[...], proj[...], 0, 1).astype(jnp.bfloat16)
    weights[...] = turned
    outgoing_sum[0] = dot(turned, picked, 1, 0).astype(jnp.bfloat16)
    enter()
    sum_start(0)
    tell(0)
    for chunk in range(1, CHUNKS):
        choose(chunk)
    value = dot(weights[...], feat[...], 1, 0).astype(jnp.bfloat16)
    projected[...] = value
    whole = dot(value, pick[:, lanes:], 1, 0).astype(jnp.bfloat16)
    for chunk in range(1, CHUNKS):
        outgoing_sum[chunk] = whole[:, (chunk - 1) * lanes : chunk * lanes]
    for load in loads[5:]:
        load.wait()
    weights_self[...] = dot(selfw[...], proj[...], 0, 1).astype(jnp.bfloat16)
    used = lax.broadcasted_iota(jnp.int32, (slot_count, nodes), 0) < degree[...]
    codes = jnp.where(used, neigh[...], -1)
    neigh[...] = codes
    depth = 256
    row_of = lax.broadcasted_iota(jnp.int32, (depth, LANES), 0).astype(jnp.float32).astype(jnp.bfloat16)
    one = jnp.ones((depth, LANES), jnp.bfloat16)
    zero = jnp.zeros((depth, LANES), jnp.bfloat16)

    def tally(index, carry):
        start = pl.multiple_of(index * depth, depth)
        for lane in range(nodes // LANES):
            there = slice(lane * LANES, (lane + 1) * LANES)
            near = jnp.clip(neigh[:, there] - start, -1, depth).astype(jnp.float32)
            total = zero
            for slot in range(slot_count):
                code = jnp.broadcast_to(near[slot : slot + 1, :], (16, LANES)).astype(jnp.bfloat16)
                code = jnp.concatenate([code] * (depth // 16), axis=0)
                total = total + jnp.where(row_of == code, one, zero)
            counts[pl.ds(start, depth), there] = total
        return carry

    lax.fori_loop(0, nodes // depth // 2, tally, 0)
    for chunk in range(1, CHUNKS):
        sum_start(chunk)
    lax.fori_loop(nodes // depth // 2, nodes // depth, tally, 0)
    share = 1.0 / degree[...].astype(jnp.float32)
    value = dot(projected[...], counts[0:nodes, :], 1, 0) * share
    value = value + dot(weights_self[...], feat[...], 1, 0)
    outgoing_self[...] = value.astype(jnp.bfloat16)
    for step in steps:
        self_copy(step).start()
    own_self[...] = outgoing_self[band(column), :].astype(jnp.float32)
    if stages:
        hear(0)
    if stages > 1:
        tell(1)

    def part_copy(peer, slot):
        return pltpu.make_async_remote_copy(
            src_ref=packed_out.at[peer],
            dst_ref=packed_in.at[slot],
            send_sem=sends.at[0],
            recv_sem=row_recv.at[slot],
            device_id=(column, peer),
            device_id_type=MESH,
        )

    half = lax.broadcasted_iota(jnp.int32, (width, LANES), 1) // capacity

    for stage in range(1, stages):
        hear(stage)
        if stage + 1 < stages:
            tell(stage + 1)

    @pl.when(part == carrier)
    def _():
        for chunk in range(CHUNKS):
            settle(incoming_sum.at[chunk, pl.ds(0, fold * cols - 1)], sum_recv.at[chunk])
            totals = []
            for place in range(fold):
                if place == fold - 1:
                    total = outgoing_sum[chunk, band(column), :].astype(jnp.float32)
                else:
                    total = incoming_sum[chunk, place * cols + column].astype(jnp.float32)
                for step in steps:
                    value = incoming_sum[chunk, place * cols + partner(column, step, cols)]
                    total = total + value.astype(jnp.float32)
                totals.append(total)
            first = chunk * rate
            for target in range(rate):
                there = slice(target // fold * LANES, (target // fold + 1) * LANES)
                tight = None
                for place in range(fold):
                    shift = (place - target % fold) * capacity % LANES
                    value = totals[place][:, there]
                    value = pltpu.roll(value, shift, 1) if shift else value
                    tight = value if tight is None else jnp.where(half == place, value, tight)
                packed_out[first + target] = tight.astype(jnp.bfloat16)
            for target in range(rate):

                @pl.when(first + target != part)
                def _():
                    part_copy(first + target, pair).start()

        packed_in[pair] = packed_out[part]

    lax.fori_loop(nodes // depth, counts.shape[0] // depth, tally, 0)
    remote[...] = jnp.zeros((width, nodes), jnp.float32)

    def gather(turn, carry):
        source = (pair + turn) % pairs

        @pl.when(source * fold + fold - 1 != part)
        def _():
            part_copy(part, source).wait_recv()

        start = pl.multiple_of(nodes + source * LANES, LANES)
        remote[...] += dot(packed_in[source], counts[pl.ds(start, LANES), :], 1, 0)
        return carry

    lax.fori_loop(0, pairs - 1, gather, 0)
    total = own_self[...]
    settle(incoming_self.at[pl.ds(0, cols - 1)], self_recv.at[0])
    for step in steps:
        total = total + incoming_self[partner(column, step, cols)].astype(jnp.float32)
    own_self[...] = total

    all_sums = cols * width * slots + (cols - 1) * width * nodes
    carried = all_sums - width * slots + (parts - 1) * width * LANES

    @pl.when(part == carrier)
    def _():
        settle(counts.at[pl.ds(0, carried // nodes)], sends.at[0])

    @pl.when(part != carrier)
    def _():
        settle(counts.at[pl.ds(0, all_sums // nodes)], sends.at[0])

    gather(pairs - 1, 0)
    result = own_self[...] + remote[...] * share
    out_ref[...] = jnp.maximum(result, 0.0).astype(out_ref.dtype)


def local(features, proj_in, self_weight, neigh_weight, neighbors, degree, send_rows, send_count):
    cols = lax.axis_size("cols")
    parts = lax.axis_size("dom")
    inputs, hid = proj_in.shape
    width = hid // cols
    nodes = features.shape[1]
    slots = send_rows.shape[1]
    capacity = slots // parts
    fold = LANES // capacity
    degree = degree.reshape(1, nodes)
    arguments = (
        features,
        proj_in,
        self_weight,
        neigh_weight,
        neighbors,
        degree,
        send_rows,
        send_count,
    )
    bf16 = jnp.bfloat16
    copies = pltpu.SemaphoreType.DMA
    limit = (16 << 20) + (slots * nodes + slots * hid + hid * nodes * 8) * 4
    return pl.pallas_call(
        functools.partial(kernel, cols, parts, capacity),
        out_shape=jax.ShapeDtypeStruct((width, nodes), bf16),
        in_specs=[pl.BlockSpec(memory_space=pltpu.HBM)] * len(arguments),
        out_specs=pl.BlockSpec(memory_space=pltpu.VMEM),
        scratch_shapes=[pltpu.VMEM(a.shape, a.dtype) for a in arguments]
        + [
            pltpu.VMEM((hid, inputs), bf16),
            pltpu.VMEM((hid, inputs), bf16),
            pltpu.VMEM((hid, nodes), bf16),
            pltpu.VMEM((width, nodes), jnp.float32),
            pltpu.VMEM((CHUNKS, hid, slots // CHUNKS), bf16),
            pltpu.VMEM((hid, nodes), bf16),
            pltpu.VMEM((CHUNKS, fold * cols, width, slots // CHUNKS), bf16),
            pltpu.VMEM((cols, width, nodes), bf16),
            pltpu.VMEM((nodes, slots), bf16),
            pltpu.VMEM((parts, width, LANES), bf16),
            pltpu.VMEM((parts // fold, width, LANES), bf16),
            pltpu.VMEM((width, nodes), jnp.float32),
            pltpu.VMEM((nodes + slots, nodes), bf16),
            copies((len(arguments),)),
            copies((1,)),
            copies((CHUNKS,)),
            copies((parts // fold,)),
            copies((1,)),
            pltpu.SemaphoreType.REGULAR((max(1, rounds(parts // fold)),)),
        ],
        compiler_params=pltpu.CompilerParams(
            collective_id=0, has_side_effects=True, vmem_limit_bytes=limit
        ),
        name="layer",
    )(*[pltpu.with_memory_space_constraint(a, pltpu.HBM) for a in arguments])


def solution(mesh):
    return jax.shard_map(
        local,
        mesh=mesh,
        in_specs=(
            P("cols", "dom"),
            P("cols", None),
            P(),
            P(),
            P(None, "dom"),
            P("dom"),
            P("dom", None),
            P("dom", None),
        ),
        out_specs=P("cols", "dom"),
        check_vma=False,
    )
```

```python
import functools

import jax
import jax.numpy as jnp
from jax import lax
from jax.experimental import pallas as pl
from jax.experimental.pallas import tpu as pltpu
from jax.sharding import PartitionSpec as P

MESH = pl.DeviceIdType.MESH
LANES = 128
CHUNKS = 4


def dot(left, right, left_dim, right_dim):
    return lax.dot_general(
        left, right, (((left_dim,), (right_dim,)), ((), ())), preferred_element_type=jnp.float32
    )


def partner(me, step, count):
    if count & (count - 1):
        return (me + step) % count
    other = me
    for bit in range(count.bit_length()):
        if step >> bit & 1:
            size = 1 << bit
            other = other + size - 2 * size * (me // size % 2)
    return other


def rounds(pairs):
    stages = 0
    while 1 << stages < pairs - 1:
        stages += 1
    return stages


def kernel(
    cols,
    parts,
    capacity,
    feat_hbm,
    proj_hbm,
    selfw_hbm,
    neighw_hbm,
    neigh_hbm,
    degree_hbm,
    rows_hbm,
    count_hbm,
    out_ref,
    feat,
    proj,
    selfw,
    neighw,
    neigh,
    degree,
    rows,
    count,
    weights,
    weights_self,
    projected,
    own_self,
    outgoing_sum,
    outgoing_self,
    incoming_sum,
    incoming_self,
    pick,
    packed_out,
    packed_in,
    remote,
    counts,
    in_sem,
    sends,
    sum_recv,
    row_recv,
    self_recv,
    known,
):
    column = lax.axis_index("cols")
    part = lax.axis_index("dom")
    width = out_ref.shape[0]
    nodes = out_ref.shape[1]
    slots = rows.shape[1]
    slot_count = neigh.shape[0]
    fold = LANES // capacity
    pairs = parts // fold
    pair = part // fold
    member = part % fold
    carrier = pair * fold + fold - 1
    steps = sorted(range(1, cols), key=lambda step: -bin(step).count("1"))

    loads = [
        pltpu.make_async_copy(source, target, in_sem.at[i])
        for i, (source, target) in enumerate(
            (
                (rows_hbm, rows),
                (count_hbm, count),
                (feat_hbm, feat),
                (neighw_hbm, neighw),
                (proj_hbm, proj),
                (selfw_hbm, selfw),
                (neigh_hbm, neigh),
                (degree_hbm, degree),
            )
        )
    ]
    for load in loads[:5]:
        load.start()

    barrier = pltpu.get_barrier_semaphore()

    def greet(target, place):
        pl.semaphore_signal(
            barrier, inc=1, device_id=(target, place), device_id_type=MESH
        )

    for step in range(cols):
        for turn in range(1 if step == 0 else 0, fold):
            greet((column + step) % cols, pair * fold + (part + turn) % fold)
    for way in (-1, 1):

        @pl.when((pair + way >= 0) & (pair + way < pairs))
        def _():
            for place in range(fold):
                greet(column, (pair + way) * fold + place)

    def enter():
        beside = (pair - 1 + pairs) // pairs + 1 - (pair + 1) // pairs
        pl.semaphore_wait(barrier, cols * fold - 1 + beside * fold)

    def aside(distance, act):
        for way, offset in enumerate((-distance, distance)):

            @pl.when((part + offset >= 0) & (part + offset < parts))
            def _():
                act(way, part + offset)

    def tell(stage):
        aside(
            fold << stage,
            lambda way, peer: pl.semaphore_signal(
                known.at[stage], inc=1, device_id=(column, peer), device_id_type=MESH
            ),
        )

    def hear(stage):
        distance = fold << stage
        sides = (part - distance + parts) // parts + 1 - (part + distance) // parts
        pl.semaphore_wait(known.at[stage], sides)

    stages = rounds(pairs)

    for load in loads[5:]:
        load.start()

    def band(index):
        return pl.ds(pl.multiple_of(index * width, width), width)

    def scatter(source, target, send, recv, peer, place):
        return pltpu.make_async_remote_copy(
            src_ref=source,
            dst_ref=target,
            send_sem=send,
            recv_sem=recv,
            device_id=(peer, place),
            device_id_type=MESH,
        )

    def sum_copy(chunk, step):
        peer = partner(column, step, cols)
        return scatter(
            outgoing_sum.at[chunk, band(peer)],
            incoming_sum.at[chunk, member * cols + column],
            sends.at[0],
            sum_recv.at[chunk],
            peer,
            carrier,
        )

    def settle(refs, semaphore):
        pltpu.make_async_copy(refs, refs, semaphore).wait()

    def sum_start(chunk):
        for step in steps:
            sum_copy(chunk, step).start()

        @pl.when(part != carrier)
        def _():
            sum_copy(chunk, 0).start()

    def self_copy(step):
        peer = partner(column, step, cols)
        return scatter(
            outgoing_self.at[band(peer)],
            incoming_self.at[column],
            sends.at[0],
            self_recv.at[0],
            peer,
            part,
        )

    lanes = slots // CHUNKS
    rate = parts // CHUNKS
    group = min(lanes, 512)

    def choose(chunk):
        amount = jnp.zeros((1, lanes), jnp.int32)
        place = lax.broadcasted_iota(jnp.int32, (1, lanes), 1)
        for index in range(rate):
            here = place // capacity == index
            peer = chunk * rate + index
            amount = jnp.where(here, count[:, peer : peer + 1], amount)
        wanted = jnp.where(
            place % capacity < amount, rows[:, chunk * lanes : (chunk + 1) * lanes], -1
        )
        for start in range(0, lanes, group):
            hit = (
                lax.broadcasted_iota(jnp.int32, (nodes, group), 0)
                == wanted[:, start : start + group]
            )
            there = slice(chunk * lanes + start, chunk * lanes + start + group)
            pick[:, there] = jnp.where(hit, 1.0, 0.0).astype(jnp.bfloat16)

    for load in loads[:2]:
        load.wait()
    choose(0)
    for load in loads[2:5]:
        load.wait()
    picked = dot(feat[...], pick[:, 0:lanes], 1, 0).astype(jnp.bfloat16)
    turned = dot(neighw[...], proj[...], 0, 1).astype(jnp.bfloat16)
    weights[...] = turned
    outgoing_sum[0] = dot(turned, picked, 1, 0).astype(jnp.bfloat16)
    enter()
    sum_start(0)
    tell(0)
    for chunk in range(1, CHUNKS):
        choose(chunk)
    value = dot(weights[...], feat[...], 1, 0).astype(jnp.bfloat16)
    projected[...] = value
    whole = dot(value, pick[:, lanes:], 1, 0).astype(jnp.bfloat16)
    for chunk in range(1, CHUNKS):
        outgoing_sum[chunk] = whole[:, (chunk - 1) * lanes : chunk * lanes]
    for load in loads[5:]:
        load.wait()
    weights_self[...] = dot(selfw[...], proj[...], 0, 1).astype(jnp.bfloat16)
    used = lax.broadcasted_iota(jnp.int32, (slot_count, nodes), 0) < degree[...]
    codes = jnp.where(used, neigh[...], -1)
    neigh[...] = codes
    depth = 256
    row_of = lax.broadcasted_iota(jnp.int32, (depth, LANES), 0).astype(jnp.float32).astype(jnp.bfloat16)
    one = jnp.ones((depth, LANES), jnp.bfloat16)
    zero = jnp.zeros((depth, LANES), jnp.bfloat16)

    def tally(index, carry):
        start = pl.multiple_of(index * depth, depth)
        for lane in range(nodes // LANES):
            there = slice(lane * LANES, (lane + 1) * LANES)
            near = jnp.clip(neigh[:, there] - start, -1, depth).astype(jnp.float32)
            total = zero
            for slot in range(slot_count):
                code = jnp.broadcast_to(near[slot : slot + 1, :], (16, LANES)).astype(jnp.bfloat16)
                code = jnp.concatenate([code] * (depth // 16), axis=0)
                total = total + jnp.where(row_of == code, one, zero)
            counts[pl.ds(start, depth), there] = total
        return carry

    lax.fori_loop(0, nodes // depth // 2, tally, 0)
    for chunk in range(1, CHUNKS - 1):
        sum_start(chunk)
    lax.fori_loop(nodes // depth // 2, nodes // depth, tally, 0)
    sum_start(CHUNKS - 1)
    share = 1.0 / degree[...].astype(jnp.float32)
    value = dot(projected[...], counts[0:nodes, :], 1, 0) * share
    value = value + dot(weights_self[...], feat[...], 1, 0)
    outgoing_self[...] = value.astype(jnp.bfloat16)
    for step in steps:
        self_copy(step).start()
    own_self[...] = outgoing_self[band(column), :].astype(jnp.float32)
    if stages:
        hear(0)
    if stages > 1:
        tell(1)

    def part_copy(peer, slot):
        return pltpu.make_async_remote_copy(
            src_ref=packed_out.at[peer],
            dst_ref=packed_in.at[slot],
            send_sem=sends.at[0],
            recv_sem=row_recv.at[slot],
            device_id=(column, peer),
            device_id_type=MESH,
        )

    half = lax.broadcasted_iota(jnp.int32, (width, LANES), 1) // capacity

    for stage in range(1, stages):
        hear(stage)
        if stage + 1 < stages:
            tell(stage + 1)

    @pl.when(part == carrier)
    def _():
        for chunk in range(CHUNKS):
            settle(incoming_sum.at[chunk, pl.ds(0, fold * cols - 1)], sum_recv.at[chunk])
            totals = []
            for place in range(fold):
                if place == fold - 1:
                    total = outgoing_sum[chunk, band(column), :].astype(jnp.float32)
                else:
                    total = incoming_sum[chunk, place * cols + column].astype(jnp.float32)
                for step in steps:
                    value = incoming_sum[chunk, place * cols + partner(column, step, cols)]
                    total = total + value.astype(jnp.float32)
                totals.append(total)
            first = chunk * rate
            for target in range(rate):
                there = slice(target // fold * LANES, (target // fold + 1) * LANES)
                tight = None
                for place in range(fold):
                    shift = (place - target % fold) * capacity % LANES
                    value = totals[place][:, there]
                    value = pltpu.roll(value, shift, 1) if shift else value
                    tight = value if tight is None else jnp.where(half == place, value, tight)
                packed_out[first + target] = tight.astype(jnp.bfloat16)
            for target in range(rate):

                @pl.when(first + target != part)
                def _():
                    part_copy(first + target, pair).start()

        packed_in[pair] = packed_out[part]

    lax.fori_loop(nodes // depth, counts.shape[0] // depth, tally, 0)
    remote[...] = jnp.zeros((width, nodes), jnp.float32)

    def gather(turn, carry):
        source = (pair + turn) % pairs

        @pl.when(source * fold + fold - 1 != part)
        def _():
            part_copy(part, source).wait_recv()

        start = pl.multiple_of(nodes + source * LANES, LANES)
        remote[...] += dot(packed_in[source], counts[pl.ds(start, LANES), :], 1, 0)
        return carry

    lax.fori_loop(0, pairs - 1, gather, 0)
    total = own_self[...]
    settle(incoming_self.at[pl.ds(0, cols - 1)], self_recv.at[0])
    for step in steps:
        total = total + incoming_self[partner(column, step, cols)].astype(jnp.float32)
    own_self[...] = total

    all_sums = cols * width * slots + (cols - 1) * width * nodes
    carried = all_sums - width * slots + (parts - 1) * width * LANES

    @pl.when(part == carrier)
    def _():
        settle(counts.at[pl.ds(0, carried // nodes)], sends.at[0])

    @pl.when(part != carrier)
    def _():
        settle(counts.at[pl.ds(0, all_sums // nodes)], sends.at[0])

    gather(pairs - 1, 0)
    result = own_self[...] + remote[...] * share
    out_ref[...] = jnp.maximum(result, 0.0).astype(out_ref.dtype)


def local(features, proj_in, self_weight, neigh_weight, neighbors, degree, send_rows, send_count):
    cols = lax.axis_size("cols")
    parts = lax.axis_size("dom")
    inputs, hid = proj_in.shape
    width = hid // cols
    nodes = features.shape[1]
    slots = send_rows.shape[1]
    capacity = slots // parts
    fold = LANES // capacity
    degree = degree.reshape(1, nodes)
    arguments = (
        features,
        proj_in,
        self_weight,
        neigh_weight,
        neighbors,
        degree,
        send_rows,
        send_count,
    )
    bf16 = jnp.bfloat16
    copies = pltpu.SemaphoreType.DMA
    limit = (16 << 20) + (slots * nodes + slots * hid + hid * nodes * 8) * 4
    return pl.pallas_call(
        functools.partial(kernel, cols, parts, capacity),
        out_shape=jax.ShapeDtypeStruct((width, nodes), bf16),
        in_specs=[pl.BlockSpec(memory_space=pltpu.HBM)] * len(arguments),
        out_specs=pl.BlockSpec(memory_space=pltpu.VMEM),
        scratch_shapes=[pltpu.VMEM(a.shape, a.dtype) for a in arguments]
        + [
            pltpu.VMEM((hid, inputs), bf16),
            pltpu.VMEM((hid, inputs), bf16),
            pltpu.VMEM((hid, nodes), bf16),
            pltpu.VMEM((width, nodes), jnp.float32),
            pltpu.VMEM((CHUNKS, hid, slots // CHUNKS), bf16),
            pltpu.VMEM((hid, nodes), bf16),
            pltpu.VMEM((CHUNKS, fold * cols, width, slots // CHUNKS), bf16),
            pltpu.VMEM((cols, width, nodes), bf16),
            pltpu.VMEM((nodes, slots), bf16),
            pltpu.VMEM((parts, width, LANES), bf16),
            pltpu.VMEM((parts // fold, width, LANES), bf16),
            pltpu.VMEM((width, nodes), jnp.float32),
            pltpu.VMEM((nodes + slots, nodes), bf16),
            copies((len(arguments),)),
            copies((1,)),
            copies((CHUNKS,)),
            copies((parts // fold,)),
            copies((1,)),
            pltpu.SemaphoreType.REGULAR((max(1, rounds(parts // fold)),)),
        ],
        compiler_params=pltpu.CompilerParams(
            collective_id=0, has_side_effects=True, vmem_limit_bytes=limit
        ),
        name="layer",
    )(*[pltpu.with_memory_space_constraint(a, pltpu.HBM) for a in arguments])


def solution(mesh):
    return jax.shard_map(
        local,
        mesh=mesh,
        in_specs=(
            P("cols", "dom"),
            P("cols", None),
            P(),
            P(),
            P(None, "dom"),
            P("dom"),
            P("dom", None),
            P("dom", None),
        ),
        out_specs=P("cols", "dom"),
        check_vma=False,
    )
```
